128 devices in a mesh: strike: 32 (over y, x, z_lo), depth: 4 (over z_hi, core).
Axes of the slice: x: 4, y: 4, z: 4 (z_hi: 2, z_lo: 2; z = z_hi * 2 + z_lo), core: 2. Of those that a mesh axis runs over, the one named last changes fastest.
Arguments:
- fault_slip: float32 [16384, 2048], P('strike', 'depth'), may hold values from -6 to 6
- rate_prev: float32 [16384, 2048], P('strike', 'depth'), may hold values from -1 to 3
- log_state: float32 [16384, 2048], P('strike', 'depth'), may hold values from -2 to 2
- weakening: float32 [16384, 2048], P('strike', 'depth'), may hold values from 0.5 to 2
- strength: float32 [16384, 2048], P('strike', 'depth'), may hold values from 0.25 to 2.5
- pre_stress: float32 [16384, 2048], P('strike', 'depth'), may hold values from 1 to 3
- kernel: float32 [9, 1024, 16384], P(None, ('strike', 'depth')), may hold values from -2 to 2
- history: float32 [8, 2, 1024, 16384], P(None, None, ('strike', 'depth')), may hold values from -6 to 6
Outputs:
- velocity: float32 [16384, 2048], P('strike', 'depth')
- new_slip: float32 [16384, 2048], P('strike', 'depth')
- slip_modes: float32 [2, 1024, 16384], P(None, ('strike', 'depth'))
The draws below stay inside these ranges and needn't reach their ends.
All inputs are finite; a program needn't handle non-finite values.
Results may differ from the reference program's by a relative error of at most 0.0003.
Values sent between devices are 32-bit elements; how exact they have to be, the bound alone decides.
No kernel may reach another device: no remote copies, remote signals or barrier semaphores. Data moves between devices by JAX's collectives and lax.ppermute only.
A program may use at most 128 MiB of HBM per device.

```python
import math
import jax
import jax.numpy as jnp
from jax import lax

NS = 16384
ND = 2048
LAGS = 8
NEWTON_ITERS = 4
MODES = 1024


def block_levels(stream_key, dims, cuts, low, top_value):
    gain, own = 1.0, jax.random.fold_in(stream_key, 6)
    for axis_at, blocks in cuts:
        draws = jnp.exp(jax.random.uniform(jax.random.fold_in(own, axis_at), (blocks,), jnp.float32, low / len(cuts), top_value / len(cuts)))
        gain = gain * jnp.repeat(draws, dims[axis_at] // blocks).reshape([-1 if axis == axis_at else 1 for axis in range(len(dims))])
    return gain


def bell_draw(key, shape, width, reach, pieces=(), dtype=jnp.bfloat16):
    result = jax.random.normal(key, shape, jnp.float32) * width
    if len(pieces) > 0:
        result = block_levels(key, shape, pieces, -0.22, 0.18) * result
    return jnp.clip(result, min=-reach, max=reach).astype(dtype)


def setup_inputs(seed: int = 0) -> dict:
    streams_of = jax.random.split(jax.random.key(seed), 9)
    fault_slip = bell_draw(streams_of[0], (NS, ND), 1.0, 6.0, ((0, 32), (1, 4)), jnp.float32)
    rate_prev = jnp.clip(-1.0 + 4.0 * jax.random.uniform(streams_of[1], (NS, ND), jnp.float32) ** block_levels(streams_of[1], (NS, ND), ((0, 32), (1, 4)), -0.2, 0.2), -1.0, 3.0)
    log_state = jnp.clip(jax.random.uniform(streams_of[2], (NS, ND), jnp.float32, -2.0, 2.0) * block_levels(streams_of[2], (NS, ND), ((0, 32), (1, 4)), -0.4, 0.0), -2.0, 2.0)
    weakening = jnp.clip(jnp.exp(math.log(2.0) - 1.3862944 * jax.random.uniform(streams_of[3], (NS, ND), jnp.float32) ** block_levels(streams_of[3], (NS, ND), ((0, 32), (1, 4)), -0.2, 0.2)), 0.5, 2.0)
    strength = jnp.clip(jnp.exp(math.log(2.5) - 2.3025851 * jax.random.uniform(streams_of[4], (NS, ND), jnp.float32) ** block_levels(streams_of[4], (NS, ND), ((0, 32), (1, 4)), -0.2, 0.2)), 0.25, 2.5)
    pre_stress = jnp.clip(1.0 + 2.0 * jax.random.uniform(streams_of[5], (NS, ND), jnp.float32) ** block_levels(streams_of[5], (NS, ND), ((0, 32), (1, 4)), -0.2, 0.2), 1.0, 3.0)
    kernel = bell_draw(streams_of[6], (LAGS + 1, MODES, NS), (LAGS + 1) ** -0.5, 2.0, ((1, 128),), jnp.float32)
    history = bell_draw(streams_of[7], (LAGS, 2, MODES, NS), 1.0, 6.0, ((2, 128),), jnp.float32)
    return {"fault_slip": fault_slip, "rate_prev": rate_prev, "log_state": log_state, "weakening": weakening, "strength": strength, "pre_stress": pre_stress, "kernel": kernel, "history": history}


DAMPING = 0.5
RELAXATION = 0.5
ADVANCE = 0.5

def inverse_sinh(value):
    magnitude = jnp.abs(value)
    positive = jnp.log(magnitude + jnp.sqrt(1.0 + magnitude * magnitude))
    return jnp.where(value < 0, -positive, positive)

def friction_rate(total_stress, rate_prev, weakening, log_state, strength):
    scaling = 0.5 * jnp.exp(weakening * log_state)
    rate_now = rate_prev
    for sweep in range(NEWTON_ITERS):
        scaled = rate_now * scaling
        residual = total_stress - DAMPING * rate_now - strength * inverse_sinh(scaled)
        slope_now = -DAMPING - strength * scaling / jnp.sqrt(1.0 + scaled * scaled)
        rate_now = rate_now - RELAXATION * residual / slope_now
    return rate_now

def reference(fault_slip, rate_prev, log_state, weakening, strength, pre_stress, kernel, history):
    half_spectrum = jnp.fft.rfft(fault_slip, axis=1, norm='ortho')[:, :MODES]
    full_spectrum = jnp.fft.fft(half_spectrum, axis=0, norm='ortho')
    slip_modes = jnp.stack([jnp.real(full_spectrum).T, jnp.imag(full_spectrum).T]).astype(jnp.float32)
    spectrum = kernel[0][None] * slip_modes
    for lag_index in range(LAGS):
        spectrum = spectrum + kernel[lag_index + 1][None] * history[lag_index]
    joined = lax.complex(spectrum[0], spectrum[1]).T
    joined = jnp.fft.ifft(joined, axis=0, norm='ortho')
    joined = jnp.pad(joined, ((0, 0), (0, 1)))
    elastic = jnp.fft.irfft(joined, n=ND, axis=1, norm='ortho').astype(jnp.float32)
    velocity = friction_rate(pre_stress + elastic, rate_prev, weakening, log_state, strength)
    return (velocity, fault_slip + ADVANCE * velocity, slip_modes)
```

```python
import functools
import math

import jax
import jax.numpy as jnp
import ml_dtypes
import numpy as np
from jax import lax
from jax.experimental import pallas as pl
from jax.experimental.pallas import tpu as pltpu
from jax.sharding import PartitionSpec as P

NEWTON_ITERS = 4
DAMPING = 0.5
RELAXATION = 0.5
ADVANCE = 0.5
LAGS = 8
ALL = ("strike", "depth")
F32 = jnp.float32
BF16 = jnp.bfloat16
NN = (((1,), (0,)), ((), ()))
NT = (((1,), (1,)), ((), ()))
TN = (((0,), (0,)), ((), ()))
VMEM = pl.BlockSpec(memory_space=pltpu.VMEM)


def split_np(table):
    high = table.astype(ml_dtypes.bfloat16)
    low = (table - high.astype(np.float64)).astype(ml_dtypes.bfloat16)
    return high, low


def split(value):
    high = value.astype(BF16)
    return high, (value - high.astype(F32)).astype(BF16)


def dot3(left, right, dims):
    mul = functools.partial(lax.dot_general, dimension_numbers=dims, preferred_element_type=F32)
    return mul(left[0], right[0]) + (mul(left[0], right[1]) + mul(left[1], right[0]))


def depth_seeds(depth_len, blocks):
    cells = depth_len // 4
    cell = np.arange(cells)
    turn = 2.0 * np.pi / depth_len
    coarse = turn * ((8 * np.arange(blocks)[:, None] * cell[None]) % depth_len)
    fine = turn * ((np.arange(8)[:, None] * cell[None]) % depth_len)
    pack = lambda angle: np.stack([np.cos(angle), np.sin(angle)]).astype(np.float32)
    return pack(coarse), pack(fine)


def table_kernel(coarse_ref, fine_ref, high_ref, low_ref):
    blocks = coarse_ref.shape[1]
    cos_a, sin_a = coarse_ref[0], coarse_ref[1]
    for cls in range(4):
        for half in range(2):
            row = 4 * half + cls
            cos_b, sin_b = fine_ref[0, row : row + 1, :], fine_ref[1, row : row + 1, :]
            for part, value in enumerate(
                (cos_a * cos_b - sin_a * sin_b, sin_a * cos_b + cos_a * sin_b)
            ):
                high, low = split(value)
                rows = pl.ds((part * 2 + half) * blocks, blocks)
                high_ref[cls, rows, :] = high
                low_ref[cls, rows, :] = low


def depth_tables(depth_len, blocks):
    coarse, fine = depth_seeds(depth_len, blocks)
    shape = jax.ShapeDtypeStruct((4, 4 * blocks, depth_len // 4), BF16)
    return pl.pallas_call(
        table_kernel,
        out_shape=(shape, shape),
        in_specs=[VMEM, VMEM],
        out_specs=(VMEM, VMEM),
        name="depth_tables",
        cost_estimate=pl.CostEstimate(flops=10_000_000, bytes_accessed=5_000_000, transcendentals=0),
    )(coarse, fine)


def depth_forward_kernel(x_ref, high_ref, low_ref, out_ref):
    rows = x_ref.shape[1]
    blocks = high_ref.shape[1] // 4
    a, b, c, d = x_ref[0], x_ref[1], x_ref[2], x_ref[3]
    even, odd = a + c, b + d
    both = jnp.concatenate([a - c, b - d], axis=0)

    def put(cls, real, imag):
        for plane, value in enumerate((real, imag)):
            for half in range(2):
                start = plane * 8 + half * 4 + cls
                out_ref[pl.ds(start, blocks, stride=16), :] = value[half * blocks : (half + 1) * blocks]

    top = 2 * blocks
    for cls, value in ((0, even + odd), (2, even - odd)):
        res = dot3((high_ref[cls], low_ref[cls]), split(value), NT)
        put(cls, res[:top], -res[top:])
    parts = split(both)
    res = dot3((high_ref[1], low_ref[1]), parts, NT)
    put(1, res[:top, :rows] - res[top:, rows:], -(res[top:, :rows] + res[:top, rows:]))
    res = dot3((high_ref[3], low_ref[3]), parts, NT)
    put(3, res[:top, :rows] + res[top:, rows:], res[:top, rows:] - res[top:, :rows])


def depth_forward(lines, tables):
    blocks = tables[0].shape[1] // 4
    return pl.pallas_call(
        depth_forward_kernel,
        out_shape=jax.ShapeDtypeStruct((blocks * 16, lines.shape[1]), F32),
        in_specs=[VMEM] * 3,
        out_specs=VMEM,
        name="depth_forward",
        cost_estimate=pl.CostEstimate(flops=1_600_000_000, bytes_accessed=6_000_000, transcendentals=0),
    )(lines, *tables)


def depth_inverse_kernel(y_ref, high_ref, low_ref, out_ref):
    rows = y_ref.shape[1]
    blocks = high_ref.shape[1] // 4

    def get(cls, plane):
        return jnp.concatenate(
            [y_ref[pl.ds(plane * 8 + half * 4 + cls, blocks, stride=16), :] for half in range(2)],
            axis=0,
        )

    def turn(cls, value):
        return dot3(split(value), (high_ref[cls], low_ref[cls]), TN)

    real, imag = get(0, 0), get(0, 1)
    first = lax.broadcasted_iota(jnp.int32, real.shape, 0) == 0
    real = jnp.where(first, 0.5 * real, real)
    imag = jnp.where(first, 0.5 * imag, imag)
    zero = turn(0, jnp.concatenate([real, -imag], axis=0))
    two = turn(2, jnp.concatenate([get(2, 0), -get(2, 1)], axis=0))
    real, imag = get(1, 0), get(1, 1)
    one = turn(
        1,
        jnp.concatenate(
            [jnp.concatenate([real, -imag], axis=0), jnp.concatenate([-imag, -real], axis=0)], axis=1
        ),
    )
    real, imag = get(3, 0), get(3, 1)
    odd = one + turn(
        3,
        jnp.concatenate(
            [jnp.concatenate([real, -imag], axis=0), jnp.concatenate([imag, real], axis=0)], axis=1
        ),
    )
    plus, minus = zero + two, zero - two
    out_ref[0] = plus + odd[:rows]
    out_ref[1] = minus + odd[rows:]
    out_ref[2] = plus - odd[:rows]
    out_ref[3] = minus - odd[rows:]


def depth_inverse(waves, tables):
    return pl.pallas_call(
        depth_inverse_kernel,
        out_shape=jax.ShapeDtypeStruct((4, waves.shape[1], tables[0].shape[2]), F32),
        in_specs=[VMEM] * 3,
        out_specs=VMEM,
        name="depth_inverse",
        cost_estimate=pl.CostEstimate(flops=1_600_000_000, bytes_accessed=6_000_000, transcendentals=0),
    )(waves, *tables)


def strike_tables(edge, scale):
    turn = 2.0 * np.pi / edge
    angle = turn * (np.outer(np.arange(edge), np.arange(edge)) % edge)
    cosine, sine = np.cos(angle), np.sin(angle)
    forward = np.block([[cosine, sine], [-sine, cosine]])
    twist = 2.0 * np.pi / (edge * edge) * np.outer(np.arange(edge), np.arange(edge))
    twist = np.stack([np.cos(twist), np.sin(twist)]) * scale
    return (*split_np(forward), *split_np(forward.T), twist.astype(np.float32))


def strike_kernel(
    x_ref, gain_ref, past_ref, fh_ref, fl_ref, bh_ref, bl_ref, twist_ref, modes_ref, out_ref, held
):
    edge = twist_ref.shape[1]
    forward = (fh_ref[...], fl_ref[...])
    backward = (bh_ref[...], bl_ref[...])
    cosine, sine = twist_ref[0], twist_ref[1]
    lanes = lambda value, m: value[:, m * edge : (m + 1) * edge]

    def gather(ref, m):
        return jnp.concatenate(
            [ref[pl.ds(plane * 8 + m, edge, stride=16), :] for plane in range(2)], axis=0
        )

    value = jnp.concatenate([gather(x_ref, m) for m in range(8)], axis=1)
    first = dot3(forward, split(value), NN)
    turned = []
    for m in range(8):
        part = lanes(first, m)
        real, imag = part[:edge], part[edge:]
        turned.append(
            jnp.concatenate([real * cosine + imag * sine, imag * cosine - real * sine], axis=1)
        )
    modes = dot3(forward, split(jnp.concatenate(turned, axis=0)), NT)
    for plane in range(2):
        for m in range(8):
            held[plane, pl.ds(m, edge, stride=8), :] = lanes(modes, m)[plane * edge : (plane + 1) * edge]
    spectrum = []
    for m in range(8):
        part = lanes(modes, m)
        rows = pl.ds(m, edge, stride=8)
        gain = gain_ref[rows, :]
        spectrum.append(
            jnp.concatenate(
                [gain * part[:edge] + past_ref[0, rows, :], gain * part[edge:] + past_ref[1, rows, :]],
                axis=0,
            )
        )
    third = dot3(backward, split(jnp.concatenate(spectrum, axis=1)), NN)
    turned = []
    for m in range(8):
        part = lanes(third, m)
        real, imag = part[:edge], part[edge:]
        turned.append(
            jnp.concatenate(
                [2.0 * (real * cosine - imag * sine), 2.0 * (imag * cosine + real * sine)], axis=1
            )
        )
    last = dot3(backward, split(jnp.concatenate(turned, axis=0)), NT)
    for plane in range(2):
        for m in range(8):
            out_ref[pl.ds(plane * 8 + m, edge, stride=16), :] = lanes(last, m)[
                plane * edge : (plane + 1) * edge
            ]
        for k in range(edge):
            modes_ref[plane, :, k * edge : (k + 1) * edge] = held[plane, k * 8 : (k + 1) * 8, :]


def strike_both(pencil, gain, past, tables):
    edge = tables[-1].shape[1]
    return pl.pallas_call(
        strike_kernel,
        out_shape=(
            jax.ShapeDtypeStruct((2, 8, edge * edge), F32),
            jax.ShapeDtypeStruct((edge * 16, edge), F32),
        ),
        in_specs=[VMEM] * 8,
        out_specs=(VMEM, VMEM),
        scratch_shapes=[pltpu.VMEM((2, edge * 8, edge), F32)],
        name="strike_both",
        cost_estimate=pl.CostEstimate(flops=1_600_000_000, bytes_accessed=6_000_000, transcendentals=0),
    )(pencil, gain, past, *tables)


def past_kernel(kernel_ref, history_ref, gain_ref, past_ref):
    tiles = kernel_ref.shape[2] // 128
    for tile in range(tiles):
        cols = pl.ds(tile * 128, 128)
        rows = pl.ds(tile * 8, 8)
        gain_ref[rows, :] = kernel_ref[0, :, cols]
        for plane in range(2):
            total = kernel_ref[1, :, cols] * history_ref[0, plane, :, cols]
            for lag in range(1, LAGS):
                total = total + kernel_ref[lag + 1, :, cols] * history_ref[lag, plane, :, cols]
            past_ref[plane, rows, :] = total


def past_sum(kernel, history):
    length = kernel.shape[2]
    block = 2048
    return pl.pallas_call(
        past_kernel,
        grid=(length // block,),
        out_shape=(
            jax.ShapeDtypeStruct((length // 16, 128), F32),
            jax.ShapeDtypeStruct((2, length // 16, 128), F32),
        ),
        in_specs=[
            pl.BlockSpec((LAGS + 1, 8, block), lambda i: (0, 0, i)),
            pl.BlockSpec((LAGS, 2, 8, block), lambda i: (0, 0, 0, i)),
        ],
        out_specs=(
            pl.BlockSpec((block // 16, 128), lambda i: (i, 0)),
            pl.BlockSpec((2, block // 16, 128), lambda i: (0, i, 0)),
        ),
        name="past_sum",
        cost_estimate=pl.CostEstimate(flops=4_200_000, bytes_accessed=14_700_000, transcendentals=0),
    )(kernel, history)


def inverse_sinh(value):
    magnitude = jnp.abs(value)
    positive = jnp.log(magnitude + jnp.sqrt(1.0 + magnitude * magnitude))
    return jnp.where(value < 0, -positive, positive)


def friction_rate(total_stress, rate_prev, weakening, log_state, strength):
    scaling = 0.5 * jnp.exp(weakening * log_state)
    rate_now = rate_prev
    for sweep in range(NEWTON_ITERS):
        scaled = rate_now * scaling
        residual = total_stress - DAMPING * rate_now - strength * inverse_sinh(scaled)
        slope_now = -DAMPING - strength * scaling / jnp.sqrt(1.0 + scaled * scaled)
        rate_now = rate_now - RELAXATION * residual / slope_now
    return rate_now


def body(fault_slip, rate_prev, log_state, weakening, strength, pre_stress, kernel, history):
    rows, cells = fault_slip.shape
    depth_size = lax.axis_size("depth")
    devices = lax.axis_size("strike") * depth_size
    edge = rows // depth_size
    depth_len = cells * depth_size
    tables = depth_tables(depth_len, devices)
    lines = lax.all_to_all(fault_slip.reshape(depth_size, edge, cells), "depth", 0, 0)
    gain, past = past_sum(kernel, history)
    waves = depth_forward(lines, tables)
    pencil = lax.all_to_all(waves.reshape(devices, 16, edge), ALL, 0, 0)
    scale = 1.0 / math.sqrt(depth_len * edge * devices)
    slip_modes, waves = strike_both(
        pencil.reshape(devices * 16, edge), gain, past, strike_tables(edge, scale)
    )
    waves = lax.all_to_all(waves.reshape(devices, 16, edge), ALL, 0, 0)
    cell_rows = depth_inverse(waves.reshape(devices * 16, edge), tables)
    elastic = lax.all_to_all(cell_rows, "depth", 0, 0).reshape(rows, cells)
    velocity = friction_rate(pre_stress + elastic, rate_prev, weakening, log_state, strength)
    return (velocity, fault_slip + ADVANCE * velocity, slip_modes)


def solution(mesh):
    return jax.shard_map(
        body,
        mesh=mesh,
        in_specs=(
            P("strike", "depth"),
            P("strike", "depth"),
            P("strike", "depth"),
            P("strike", "depth"),
            P("strike", "depth"),
            P("strike", "depth"),
            P(None, ("strike", "depth"), None),
            P(None, None, ("strike", "depth"), None),
        ),
        out_specs=(P("strike", "depth"), P("strike", "depth"), P(None, ("strike", "depth"), None)),
        check_vma=False,
    )
```

```python
import functools
import math

import jax
import jax.numpy as jnp
import ml_dtypes
import numpy as np
from jax import lax
from jax.experimental import pallas as pl
from jax.experimental.pallas import tpu as pltpu
from jax.sharding import PartitionSpec as P

NEWTON_ITERS = 4
DAMPING = 0.5
RELAXATION = 0.5
ADVANCE = 0.5
LAGS = 8
FORWARD = ((0, 384), (384, 128))
INVERSE = ((0, 128), (128, 256), (384, 128))
GRANT = 16 << 20
WIDE = 24 << 20
ALL = ("strike", "depth")
F32 = jnp.float32
BF16 = jnp.bfloat16
NN = (((1,), (0,)), ((), ()))
NT = (((1,), (1,)), ((), ()))
TN = (((0,), (0,)), ((), ()))
VMEM = pl.BlockSpec(memory_space=pltpu.VMEM)
SMEM = pl.BlockSpec(memory_space=pltpu.SMEM)
HBM = pl.BlockSpec(memory_space=pltpu.HBM)


def split_np(table):
    high = table.astype(ml_dtypes.bfloat16)
    low = (table - high.astype(np.float64)).astype(ml_dtypes.bfloat16)
    return high, low


def split(value):
    high = value.astype(BF16)
    return high, (value - high.astype(F32)).astype(BF16)


def in_hbm(*values):
    return [pltpu.with_memory_space_constraint(jnp.asarray(v), pltpu.HBM) for v in values]


def dot3(left, right, dims):
    mul = functools.partial(lax.dot_general, dimension_numbers=dims, preferred_element_type=F32)
    return mul(left[0], right[0]) + (mul(left[0], right[1]) + mul(left[1], right[0]))


def depth_seeds(depth_len, blocks):
    cells = depth_len // 4
    cell = np.arange(cells)
    turn = 2.0 * np.pi / depth_len
    coarse = turn * ((8 * np.arange(blocks)[:, None] * cell[None]) % depth_len)
    fine = turn * ((np.arange(8)[:, None] * cell[None]) % depth_len)
    pack = lambda angle: np.stack([np.cos(angle), np.sin(angle)]).astype(np.float32)
    return pack(coarse), pack(fine)


def table_kernel(coarse_ref, fine_ref, high_ref, low_ref):
    blocks = coarse_ref.shape[1]
    cos_a, sin_a = coarse_ref[0], coarse_ref[1]
    for cls in range(4):
        for half in range(2):
            row = 4 * half + cls
            cos_b, sin_b = fine_ref[0, row : row + 1, :], fine_ref[1, row : row + 1, :]
            for part, value in enumerate(
                (cos_a * cos_b - sin_a * sin_b, sin_a * cos_b + cos_a * sin_b)
            ):
                high, low = split(value)
                rows = pl.ds((part * 2 + half) * blocks, blocks)
                high_ref[cls, rows, :] = high
                low_ref[cls, rows, :] = low


def depth_tables(depth_len, blocks):
    coarse, fine = depth_seeds(depth_len, blocks)
    shape = jax.ShapeDtypeStruct((4, 4 * blocks, depth_len // 4), BF16)
    return pl.pallas_call(
        table_kernel,
        out_shape=(shape, shape),
        in_specs=[VMEM, VMEM],
        out_specs=(VMEM, VMEM),
        compiler_params=pltpu.CompilerParams(vmem_limit_bytes=GRANT),
        name="depth_tables",
        cost_estimate=pl.CostEstimate(flops=10_000_000, bytes_accessed=5_000_000, transcendentals=0),
    )(coarse, fine)


def depth_forward_kernel(first, column, me_ref, own_ref, one_ref, two_ref, three_ref, high_ref, low_ref, *refs):
    rows, cells = own_ref.shape
    blocks = high_ref.shape[1] // 4
    cols = pl.ds(column, cells)
    me = me_ref[0]
    swap = (me & 1) == 1
    tau = (1 - 2 * (me & 1)).astype(F32)
    sigma = (1 - (me & 2)).astype(F32)
    even, odd = own_ref[...] + two_ref[...], one_ref[...] + three_ref[...]
    left, right = sigma * (own_ref[...] - two_ref[...]), sigma * (one_ref[...] - three_ref[...])
    both = jnp.concatenate(
        [jnp.where(swap, right, left), jnp.where(swap, left, right)], axis=0
    )

    def put(cls, real, imag):
        for plane, value in enumerate((real, imag)):
            for half in range(2):
                part = value[half * blocks : (half + 1) * blocks]
                slot = cls * 4 + plane * 2 + half
                if first:
                    refs[0][slot] = part
                else:
                    start = plane * 8 + half * 4 + cls
                    refs[1][pl.ds(start, blocks, stride=16), :] = part + refs[0][slot]

    def turn(cls, parts):
        return dot3((high_ref[cls, :, cols], low_ref[cls, :, cols]), parts, NT)

    top = 2 * blocks
    for cls, value in ((0, even + odd), (2, tau * (even - odd))):
        res = turn(cls, split(value))
        put(cls, res[:top], -res[top:])
    parts = split(both)
    res = turn(1, parts)
    put(1, res[:top, :rows] - res[top:, rows:], -(res[top:, :rows] + res[:top, rows:]))
    res = turn(3, parts)
    put(3, res[:top, :rows] + res[top:, rows:], res[:top, rows:] - res[top:, :rows])


def depth_forward(column, me, parts, tables, held=None):
    blocks = tables[0].shape[1] // 4
    rows = parts[0].shape[0]
    first = held is None
    shape = (16, blocks, rows) if first else (blocks * 16, rows)
    return pl.pallas_call(
        functools.partial(depth_forward_kernel, first, column),
        out_shape=jax.ShapeDtypeStruct(shape, F32),
        in_specs=[SMEM] + [VMEM] * (6 if first else 7),
        out_specs=VMEM,
        compiler_params=pltpu.CompilerParams(vmem_limit_bytes=GRANT),
        name="depth_forward",
        cost_estimate=pl.CostEstimate(flops=1_200_000_000, bytes_accessed=4_000_000, transcendentals=0),
    )(me, *parts, *tables, *(() if first else (held,)))


def depth_inverse_kernel(column, me_ref, y_ref, high_ref, low_ref, own_ref, one_ref, two_ref, three_ref):
    rows, cells = own_ref.shape
    blocks = high_ref.shape[1] // 4
    cols = pl.ds(column, cells)
    me = me_ref[0]
    swap = (me & 1) == 1
    tau = (1 - 2 * (me & 1)).astype(F32)
    sigma = (1 - (me & 2)).astype(F32)

    def get(cls, plane):
        return jnp.concatenate(
            [y_ref[pl.ds(plane * 8 + half * 4 + cls, blocks, stride=16), :] for half in range(2)],
            axis=0,
        )

    def turn(cls, value):
        return dot3(split(value), (high_ref[cls, :, cols], low_ref[cls, :, cols]), TN)

    real, imag = get(0, 0), get(0, 1)
    first = lax.broadcasted_iota(jnp.int32, real.shape, 0) == 0
    real = jnp.where(first, 0.5 * real, real)
    imag = jnp.where(first, 0.5 * imag, imag)
    zero = turn(0, jnp.concatenate([real, -imag], axis=0))
    two = tau * turn(2, jnp.concatenate([get(2, 0), -get(2, 1)], axis=0))
    real, imag = get(1, 0), get(1, 1)
    odd = turn(
        1,
        jnp.concatenate(
            [jnp.concatenate([real, -imag], axis=0), jnp.concatenate([-imag, -real], axis=0)], axis=1
        ),
    )
    real, imag = get(3, 0), get(3, 1)
    odd = sigma * (
        odd
        + turn(
            3,
            jnp.concatenate(
                [jnp.concatenate([real, -imag], axis=0), jnp.concatenate([imag, real], axis=0)], axis=1
            ),
        )
    )
    low, high = odd[:rows], odd[rows:]
    base, turned = zero + two, jnp.where(swap, high, low)
    own_ref[...] = base + turned
    two_ref[...] = base - turned
    base, turned = zero - two, jnp.where(swap, low, high)
    one_ref[...] = base + turned
    three_ref[...] = base - turned


def depth_inverse(column, width, me, waves, tables):
    rows = waves.shape[1]
    shape = jax.ShapeDtypeStruct((rows, width), F32)
    return pl.pallas_call(
        functools.partial(depth_inverse_kernel, column),
        out_shape=(shape,) * 4,
        in_specs=[SMEM] + [VMEM] * 3,
        out_specs=(VMEM,) * 4,
        compiler_params=pltpu.CompilerParams(vmem_limit_bytes=GRANT),
        name="depth_inverse",
        cost_estimate=pl.CostEstimate(flops=1_200_000_000, bytes_accessed=4_000_000, transcendentals=0),
    )(me, waves, *tables)


def strike_tables(edge, scale):
    turn = 2.0 * np.pi / edge
    angle = turn * (np.outer(np.arange(edge), np.arange(edge)) % edge)
    waves = np.stack([*split_np(np.cos(angle)), *split_np(np.sin(angle))])
    twist = 2.0 * np.pi / (edge * edge) * np.outer(np.arange(edge), np.arange(edge))
    twist = np.stack([np.cos(twist), np.sin(twist)]) * scale
    return waves, twist.astype(np.float32)


def strike_kernel(
    x_ref, gain_hbm, past_hbm, wave_hbm, twist_hbm, modes_hbm, out_ref,
    gain_ref, past_ref, wave_ref, twist_ref, held, modes_ref, sems,
):
    edge = twist_ref.shape[1]
    pairs = ((wave_hbm, wave_ref), (twist_hbm, twist_ref), (gain_hbm, gain_ref), (past_hbm, past_ref))
    loads = [pltpu.make_async_copy(a, b, sems.at[n]) for n, (a, b) in enumerate(pairs)]
    for load in loads:
        load.start()
    lanes = lambda value, m: value[:, m * edge : (m + 1) * edge]

    def gather(ref, m):
        return jnp.concatenate(
            [ref[pl.ds(plane * 8 + m, edge, stride=16), :] for plane in range(2)], axis=0
        )

    parts = split(jnp.concatenate([gather(x_ref, m) for m in range(8)], axis=1))
    loads[0].wait()

    def block(sign, part):
        cosine, sine = wave_ref[part], wave_ref[2 + part]
        left, right = (sine, -sine) if sign > 0 else (-sine, sine)
        return jnp.concatenate(
            [jnp.concatenate([cosine, left], axis=1), jnp.concatenate([right, cosine], axis=1)], axis=0
        )

    forward = (block(1, 0), block(1, 1))
    backward = (block(-1, 0), block(-1, 1))
    first = dot3(forward, parts, NN)
    loads[1].wait()
    cosine, sine = twist_ref[0], twist_ref[1]
    turned = []
    for m in range(8):
        part = lanes(first, m)
        real, imag = part[:edge], part[edge:]
        turned.append(
            jnp.concatenate([real * cosine + imag * sine, imag * cosine - real * sine], axis=1)
        )
    modes = dot3(forward, split(jnp.concatenate(turned, axis=0)), NT)
    for plane in range(2):
        for m in range(8):
            held[plane, pl.ds(m, edge, stride=8), :] = lanes(modes, m)[plane * edge : (plane + 1) * edge]
        for k in range(edge):
            modes_ref[plane, :, k * edge : (k + 1) * edge] = held[plane, k * 8 : (k + 1) * 8, :]
    save = pltpu.make_async_copy(modes_ref, modes_hbm, sems.at[4])
    save.start()
    loads[2].wait()
    loads[3].wait()
    spectrum = []
    for m in range(8):
        part = lanes(modes, m)
        rows = pl.ds(m, edge, stride=8)
        gain = gain_ref[rows, :]
        spectrum.append(
            jnp.concatenate(
                [gain * part[:edge] + past_ref[0, rows, :], gain * part[edge:] + past_ref[1, rows, :]],
                axis=0,
            )
        )
    third = dot3(backward, split(jnp.concatenate(spectrum, axis=1)), NN)
    turned = []
    for m in range(8):
        part = lanes(third, m)
        real, imag = part[:edge], part[edge:]
        turned.append(
            jnp.concatenate(
                [2.0 * (real * cosine - imag * sine), 2.0 * (imag * cosine + real * sine)], axis=1
            )
        )
    last = dot3(backward, split(jnp.concatenate(turned, axis=0)), NT)
    for plane in range(2):
        for m in range(8):
            out_ref[pl.ds(plane * 8 + m, edge, stride=16), :] = lanes(last, m)[
                plane * edge : (plane + 1) * edge
            ]
    save.wait()


def strike_both(pencil, gain, past, tables):
    waves, twist = tables
    edge = twist.shape[1]
    modes = (2, 8, edge * edge)
    return pl.pallas_call(
        strike_kernel,
        out_shape=(
            jax.ShapeDtypeStruct(modes, F32),
            jax.ShapeDtypeStruct((edge * 16, edge), F32),
        ),
        in_specs=[VMEM] + [HBM] * 4,
        out_specs=(HBM, VMEM),
        scratch_shapes=[
            pltpu.VMEM(gain.shape, F32),
            pltpu.VMEM(past.shape, F32),
            pltpu.VMEM(waves.shape, BF16),
            pltpu.VMEM(twist.shape, F32),
            pltpu.VMEM((2, edge * 8, edge), F32),
            pltpu.VMEM(modes, F32),
            pltpu.SemaphoreType.DMA((5,)),
        ],
        compiler_params=pltpu.CompilerParams(vmem_limit_bytes=WIDE),
        name="strike_both",
        cost_estimate=pl.CostEstimate(flops=1_600_000_000, bytes_accessed=6_000_000, transcendentals=0),
    )(pencil, *in_hbm(gain, past, waves, twist))


def past_kernel(kernel_ref, history_ref, gain_ref, past_ref):
    tiles = kernel_ref.shape[2] // 128
    for tile in range(tiles):
        cols = pl.ds(tile * 128, 128)
        rows = pl.ds(tile * 8, 8)
        gain_ref[rows, :] = kernel_ref[0, :, cols]
        for plane in range(2):
            total = kernel_ref[1, :, cols] * history_ref[0, plane, :, cols]
            for lag in range(1, LAGS):
                total = total + kernel_ref[lag + 1, :, cols] * history_ref[lag, plane, :, cols]
            past_ref[plane, rows, :] = total


def past_sum(kernel, history):
    length = kernel.shape[2]
    block = 2048
    return pl.pallas_call(
        past_kernel,
        grid=(length // block,),
        out_shape=(
            jax.ShapeDtypeStruct((length // 16, 128), F32),
            jax.ShapeDtypeStruct((2, length // 16, 128), F32),
        ),
        in_specs=[
            pl.BlockSpec((LAGS + 1, 8, block), lambda i: (0, 0, i)),
            pl.BlockSpec((LAGS, 2, 8, block), lambda i: (0, 0, 0, i)),
        ],
        out_specs=(
            pl.BlockSpec((block // 16, 128), lambda i: (i, 0)),
            pl.BlockSpec((2, block // 16, 128), lambda i: (0, i, 0)),
        ),
        compiler_params=pltpu.CompilerParams(vmem_limit_bytes=WIDE),
        name="past_sum",
        cost_estimate=pl.CostEstimate(flops=4_200_000, bytes_accessed=14_700_000, transcendentals=0),
    )(*in_hbm(kernel, history))


def newton_parts(rate, scaling, strength):
    scaled = rate * scaling
    magnitude = jnp.abs(scaled)
    square = 1.0 + scaled * scaled
    inverse = lax.rsqrt(square)
    positive = jnp.log(magnitude + square * inverse)
    friction = strength * jnp.where(scaled < 0, -positive, positive)
    return friction, 1.0 + (strength * scaling) * (inverse * (1.0 / DAMPING))


STEP = RELAXATION / DAMPING


def start_kernel(rate_ref, state_ref, weak_ref, strength_ref, stress_ref, scale_ref, rest_ref, gain_ref):
    scaling = 0.5 * jnp.exp(weak_ref[...] * state_ref[...])
    rate = rate_ref[...]
    friction, divisor = newton_parts(rate, scaling, strength_ref[...])
    gain = STEP / divisor
    scale_ref[...] = scaling
    gain_ref[...] = gain
    rest_ref[...] = rate + gain * (stress_ref[...] - DAMPING * rate - friction)


def friction_start(rate_prev, log_state, weakening, strength, pre_stress):
    rows, cells = rate_prev.shape
    spec = pl.BlockSpec((64, cells), lambda i: (i, 0))
    shape = jax.ShapeDtypeStruct((rows, cells), F32)
    return pl.pallas_call(
        start_kernel,
        grid=(rows // 64,),
        out_shape=(shape,) * 3,
        in_specs=[spec] * 5,
        out_specs=(spec,) * 3,
        compiler_params=pltpu.CompilerParams(vmem_limit_bytes=GRANT),
        name="friction_start",
        cost_estimate=pl.CostEstimate(flops=20_000_000, bytes_accessed=8_000_000, transcendentals=1_000_000),
    )(rate_prev, log_state, weakening, strength, pre_stress)


def friction_kernel(
    column, me_ref, own_ref, one_ref, two_ref, three_ref, scale_ref, rest_ref, gain_ref, strength_ref,
    stress_ref, slip_ref, *refs
):
    velocity_hbm, new_hbm, velocity_ref, new_ref, sems = refs[-5:]
    edge, width = own_ref.shape
    cols = pl.ds(column, width)
    saves = []
    for slot, ref in enumerate((own_ref, one_ref, two_ref, three_ref)):
        rows = pl.ds(pl.multiple_of((me_ref[0] ^ slot) * edge, edge), edge)
        elastic = ref[...]
        scaling, strength = scale_ref[rows, cols], strength_ref[rows, cols]
        total = stress_ref[rows, cols] + elastic
        rate = rest_ref[rows, cols] + gain_ref[rows, cols] * elastic
        for sweep in range(NEWTON_ITERS - 1):
            friction, divisor = newton_parts(rate, scaling, strength)
            rate = rate + STEP * (total - DAMPING * rate - friction) / divisor
        velocity_ref[slot] = rate
        new_ref[slot] = slip_ref[rows, cols] + ADVANCE * rate
        for n, (source, target) in enumerate(((velocity_ref, velocity_hbm), (new_ref, new_hbm))):
            save = pltpu.make_async_copy(source.at[slot], target.at[rows, cols], sems.at[slot, n])
            save.start()
            saves.append(save)
    for save in saves:
        save.wait()


def friction_finish(column, me, elastic, start, strength, pre_stress, fault_slip, held=()):
    edge, width = elastic[0].shape
    shape = jax.ShapeDtypeStruct(fault_slip.shape, F32)
    count = 1 + 4 + 6
    return pl.pallas_call(
        functools.partial(friction_kernel, column),
        in_specs=[SMEM] + [VMEM] * 10 + [HBM] * len(held),
        out_specs=(HBM, HBM),
        out_shape=(shape, shape),
        scratch_shapes=[
            pltpu.VMEM((4, edge, width), F32),
            pltpu.VMEM((4, edge, width), F32),
            pltpu.SemaphoreType.DMA((4, 2)),
        ],
        input_output_aliases={count + n: n for n in range(len(held))},
        compiler_params=pltpu.CompilerParams(vmem_limit_bytes=GRANT),
        name="friction_finish",
        cost_estimate=pl.CostEstimate(flops=20_000_000, bytes_accessed=5_000_000, transcendentals=1_000_000),
    )(me, *elastic, *start, strength, pre_stress, fault_slip, *in_hbm(*held))


def exchange(parts, size):
    swap = lambda part, k: lax.ppermute(part, "depth", [(place, place ^ k) for place in range(size)])
    moved = {k: swap(parts[k], k) for k in (2, 3, 1)}
    return [parts[0]] + [moved[k] for k in (1, 2, 3)]


def body(fault_slip, rate_prev, log_state, weakening, strength, pre_stress, kernel, history):
    rows, cells = fault_slip.shape
    depth_size = lax.axis_size("depth")
    devices = lax.axis_size("strike") * depth_size
    edge = rows // depth_size
    depth_len = cells * depth_size
    place = lax.axis_index("depth")
    me = place.reshape(1)
    lines, source = [], fault_slip
    for column, width in FORWARD:
        blocks = [
            lax.dynamic_slice(source, ((place ^ k) * edge, column), (edge, width))
            for k in range(depth_size)
        ]
        source, *blocks = lax.optimization_barrier((source, *blocks))
        lines.append(exchange(blocks, depth_size))
    tables = depth_tables(depth_len, devices)
    gain, past = past_sum(kernel, history)
    start = friction_start(rate_prev, log_state, weakening, strength, pre_stress)
    waves = None
    for (column, _), parts in zip(FORWARD, lines):
        waves = depth_forward(column, me, parts, tables, waves)
    pencil = lax.all_to_all(waves.reshape(devices, 16, edge), ALL, 0, 0)
    scale = 1.0 / math.sqrt(depth_len * edge * devices)
    slip_modes, waves = strike_both(
        pencil.reshape(devices * 16, edge), gain, past, strike_tables(edge, scale)
    )
    waves = lax.all_to_all(waves.reshape(devices, 16, edge), ALL, 0, 0).reshape(devices * 16, edge)
    elastic = [
        exchange(depth_inverse(column, width, me, waves, tables), depth_size)
        for column, width in INVERSE
    ]
    out = ()
    for (column, _), parts in zip(INVERSE, elastic):
        out = friction_finish(column, me, parts, start, strength, pre_stress, fault_slip, out)
    return (*out, slip_modes)


def solution(mesh):
    return jax.shard_map(
        body,
        mesh=mesh,
        in_specs=(
            P("strike", "depth"),
            P("strike", "depth"),
            P("strike", "depth"),
            P("strike", "depth"),
            P("strike", "depth"),
            P("strike", "depth"),
            P(None, ("strike", "depth"), None),
            P(None, None, ("strike", "depth"), None),
        ),
        out_specs=(P("strike", "depth"), P("strike", "depth"), P(None, ("strike", "depth"), None)),
        check_vma=False,
    )
```

```python
import functools
import math

import jax
import jax.numpy as jnp
import ml_dtypes
import numpy as np
from jax import lax
from jax.experimental import pallas as pl
from jax.experimental.pallas import tpu as pltpu
from jax.sharding import PartitionSpec as P

NEWTON_ITERS = 4
DAMPING = 0.5
RELAXATION = 0.5
ADVANCE = 0.5
LAGS = 8
FORWARD = ((0, 256), (256, 256))
INVERSE = ((0, 256), (256, 256))
GRANT = 16 << 20
WIDE = 24 << 20
ALL = ("strike", "depth")
F32 = jnp.float32
BF16 = jnp.bfloat16
NN = (((1,), (0,)), ((), ()))
NT = (((1,), (1,)), ((), ()))
TN = (((0,), (0,)), ((), ()))
VMEM = pl.BlockSpec(memory_space=pltpu.VMEM)
SMEM = pl.BlockSpec(memory_space=pltpu.SMEM)
HBM = pl.BlockSpec(memory_space=pltpu.HBM)


def split_np(table):
    high = table.astype(ml_dtypes.bfloat16)
    low = (table - high.astype(np.float64)).astype(ml_dtypes.bfloat16)
    return high, low


def split(value):
    high = value.astype(BF16)
    return high, (value - high.astype(F32)).astype(BF16)


def in_hbm(*values):
    return [pltpu.with_memory_space_constraint(jnp.asarray(v), pltpu.HBM) for v in values]


def dot3(left, right, dims):
    mul = functools.partial(lax.dot_general, dimension_numbers=dims, preferred_element_type=F32)
    return mul(left[0], right[0]) + (mul(left[0], right[1]) + mul(left[1], right[0]))


def depth_seeds(depth_len, blocks):
    cells = depth_len // 4
    cell = np.arange(cells)
    turn = 2.0 * np.pi / depth_len
    coarse = turn * ((8 * np.arange(blocks)[:, None] * cell[None]) % depth_len)
    fine = turn * ((np.arange(8)[:, None] * cell[None]) % depth_len)
    pack = lambda angle: np.stack([np.cos(angle), np.sin(angle)]).astype(np.float32)
    return pack(coarse), pack(fine)


def table_kernel(coarse_ref, fine_ref, high_ref, low_ref):
    blocks = coarse_ref.shape[1]
    cos_a, sin_a = coarse_ref[0], coarse_ref[1]
    for cls in range(4):
        for half in range(2):
            row = 4 * half + cls
            cos_b, sin_b = fine_ref[0, row : row + 1, :], fine_ref[1, row : row + 1, :]
            for part, value in enumerate(
                (cos_a * cos_b - sin_a * sin_b, sin_a * cos_b + cos_a * sin_b)
            ):
                high, low = split(value)
                rows = pl.ds((part * 2 + half) * blocks, blocks)
                high_ref[cls, rows, :] = high
                low_ref[cls, rows, :] = low


def depth_tables(depth_len, blocks):
    coarse, fine = depth_seeds(depth_len, blocks)
    shape = jax.ShapeDtypeStruct((4, 4 * blocks, depth_len // 4), BF16)
    return pl.pallas_call(
        table_kernel,
        out_shape=(shape, shape),
        in_specs=[VMEM, VMEM],
        out_specs=(VMEM, VMEM),
        compiler_params=pltpu.CompilerParams(vmem_limit_bytes=GRANT),
        name="depth_tables",
        cost_estimate=pl.CostEstimate(flops=10_000_000, bytes_accessed=5_000_000, transcendentals=0),
    )(coarse, fine)


def depth_forward_kernel(first, column, me_ref, own_ref, one_ref, two_ref, three_ref, high_ref, low_ref, *refs):
    rows, cells = own_ref.shape
    blocks = high_ref.shape[1] // 4
    cols = pl.ds(column, cells)
    me = me_ref[0]
    swap = (me & 1) == 1
    tau = (1 - 2 * (me & 1)).astype(F32)
    sigma = (1 - (me & 2)).astype(F32)
    even, odd = own_ref[...] + two_ref[...], one_ref[...] + three_ref[...]
    left, right = sigma * (own_ref[...] - two_ref[...]), sigma * (one_ref[...] - three_ref[...])
    both = jnp.concatenate(
        [jnp.where(swap, right, left), jnp.where(swap, left, right)], axis=0
    )

    def put(cls, real, imag):
        for plane, value in enumerate((real, imag)):
            for half in range(2):
                part = value[half * blocks : (half + 1) * blocks]
                slot = cls * 4 + plane * 2 + half
                if first:
                    refs[0][slot] = part
                else:
                    start = plane * 8 + half * 4 + cls
                    refs[1][pl.ds(start, blocks, stride=16), :] = part + refs[0][slot]

    def turn(cls, parts):
        return dot3((high_ref[cls, :, cols], low_ref[cls, :, cols]), parts, NT)

    top = 2 * blocks
    for cls, value in ((0, even + odd), (2, tau * (even - odd))):
        res = turn(cls, split(value))
        put(cls, res[:top], -res[top:])
    parts = split(both)
    res = turn(1, parts)
    put(1, res[:top, :rows] - res[top:, rows:], -(res[top:, :rows] + res[:top, rows:]))
    res = turn(3, parts)
    put(3, res[:top, :rows] + res[top:, rows:], res[:top, rows:] - res[top:, :rows])


def depth_forward(column, me, parts, tables, held=None):
    blocks = tables[0].shape[1] // 4
    rows = parts[0].shape[0]
    first = held is None
    shape = (16, blocks, rows) if first else (blocks * 16, rows)
    return pl.pallas_call(
        functools.partial(depth_forward_kernel, first, column),
        out_shape=jax.ShapeDtypeStruct(shape, F32),
        in_specs=[SMEM] + [VMEM] * (6 if first else 7),
        out_specs=VMEM,
        compiler_params=pltpu.CompilerParams(vmem_limit_bytes=GRANT),
        name="depth_forward",
        cost_estimate=pl.CostEstimate(flops=1_200_000_000, bytes_accessed=4_000_000, transcendentals=0),
    )(me, *parts, *tables, *(() if first else (held,)))


def depth_inverse_kernel(column, me_ref, y_ref, high_ref, low_ref, own_ref, one_ref, two_ref, three_ref):
    rows, cells = own_ref.shape
    blocks = high_ref.shape[1] // 4
    cols = pl.ds(column, cells)
    me = me_ref[0]
    swap = (me & 1) == 1
    tau = (1 - 2 * (me & 1)).astype(F32)
    sigma = (1 - (me & 2)).astype(F32)

    def get(cls, plane):
        return jnp.concatenate(
            [y_ref[pl.ds(plane * 8 + half * 4 + cls, blocks, stride=16), :] for half in range(2)],
            axis=0,
        )

    def turn(cls, value):
        return dot3(split(value), (high_ref[cls, :, cols], low_ref[cls, :, cols]), TN)

    real, imag = get(0, 0), get(0, 1)
    first = lax.broadcasted_iota(jnp.int32, real.shape, 0) == 0
    real = jnp.where(first, 0.5 * real, real)
    imag = jnp.where(first, 0.5 * imag, imag)
    zero = turn(0, jnp.concatenate([real, -imag], axis=0))
    two = tau * turn(2, jnp.concatenate([get(2, 0), -get(2, 1)], axis=0))
    real, imag = get(1, 0), get(1, 1)
    odd = turn(
        1,
        jnp.concatenate(
            [jnp.concatenate([real, -imag], axis=0), jnp.concatenate([-imag, -real], axis=0)], axis=1
        ),
    )
    real, imag = get(3, 0), get(3, 1)
    odd = sigma * (
        odd
        + turn(
            3,
            jnp.concatenate(
                [jnp.concatenate([real, -imag], axis=0), jnp.concatenate([imag, real], axis=0)], axis=1
            ),
        )
    )
    low, high = odd[:rows], odd[rows:]
    base, turned = zero + two, jnp.where(swap, high, low)
    own_ref[...] = base + turned
    two_ref[...] = base - turned
    base, turned = zero - two, jnp.where(swap, low, high)
    one_ref[...] = base + turned
    three_ref[...] = base - turned


def depth_inverse(column, width, me, waves, tables):
    rows = waves.shape[1]
    shape = jax.ShapeDtypeStruct((rows, width), F32)
    return pl.pallas_call(
        functools.partial(depth_inverse_kernel, column),
        out_shape=(shape,) * 4,
        in_specs=[SMEM] + [VMEM] * 3,
        out_specs=(VMEM,) * 4,
        compiler_params=pltpu.CompilerParams(vmem_limit_bytes=GRANT),
        name="depth_inverse",
        cost_estimate=pl.CostEstimate(flops=1_200_000_000, bytes_accessed=4_000_000, transcendentals=0),
    )(me, waves, *tables)


def strike_tables(edge, scale):
    turn = 2.0 * np.pi / edge
    angle = turn * (np.outer(np.arange(edge), np.arange(edge)) % edge)
    waves = np.stack([*split_np(np.cos(angle)), *split_np(np.sin(angle))])
    twist = 2.0 * np.pi / (edge * edge) * np.outer(np.arange(edge), np.arange(edge))
    twist = np.stack([np.cos(twist), np.sin(twist)]) * scale
    return waves, twist.astype(np.float32)


def strike_kernel(
    x_ref, gain_hbm, past_hbm, wave_ref, twist_ref, modes_hbm, out_ref,
    gain_ref, past_ref, held, modes_ref, sems,
):
    edge = twist_ref.shape[1]
    pairs = ((gain_hbm, gain_ref), (past_hbm, past_ref))
    loads = [pltpu.make_async_copy(a, b, sems.at[n]) for n, (a, b) in enumerate(pairs)]
    for load in loads:
        load.start()
    lanes = lambda value, m: value[:, m * edge : (m + 1) * edge]

    def gather(ref, m):
        return jnp.concatenate(
            [ref[pl.ds(plane * 8 + m, edge, stride=16), :] for plane in range(2)], axis=0
        )

    parts = split(jnp.concatenate([gather(x_ref, m) for m in range(8)], axis=1))

    def block(sign, part):
        cosine, sine = wave_ref[part], wave_ref[2 + part]
        left, right = (sine, -sine) if sign > 0 else (-sine, sine)
        return jnp.concatenate(
            [jnp.concatenate([cosine, left], axis=1), jnp.concatenate([right, cosine], axis=1)], axis=0
        )

    forward = (block(1, 0), block(1, 1))
    backward = (block(-1, 0), block(-1, 1))
    first = dot3(forward, parts, NN)
    cosine, sine = twist_ref[0], twist_ref[1]
    turned = []
    for m in range(8):
        part = lanes(first, m)
        real, imag = part[:edge], part[edge:]
        turned.append(
            jnp.concatenate([real * cosine + imag * sine, imag * cosine - real * sine], axis=1)
        )
    modes = dot3(forward, split(jnp.concatenate(turned, axis=0)), NT)
    for plane in range(2):
        for m in range(8):
            held[plane, pl.ds(m, edge, stride=8), :] = lanes(modes, m)[plane * edge : (plane + 1) * edge]
        for k in range(edge):
            modes_ref[plane, :, k * edge : (k + 1) * edge] = held[plane, k * 8 : (k + 1) * 8, :]
    save = pltpu.make_async_copy(modes_ref, modes_hbm, sems.at[2])
    save.start()
    for load in loads:
        load.wait()
    spectrum = []
    for m in range(8):
        part = lanes(modes, m)
        rows = pl.ds(m, edge, stride=8)
        gain = gain_ref[rows, :]
        spectrum.append(
            jnp.concatenate(
                [gain * part[:edge] + past_ref[0, rows, :], gain * part[edge:] + past_ref[1, rows, :]],
                axis=0,
            )
        )
    third = dot3(backward, split(jnp.concatenate(spectrum, axis=1)), NN)
    turned = []
    for m in range(8):
        part = lanes(third, m)
        real, imag = part[:edge], part[edge:]
        turned.append(
            jnp.concatenate(
                [2.0 * (real * cosine - imag * sine), 2.0 * (imag * cosine + real * sine)], axis=1
            )
        )
    last = dot3(backward, split(jnp.concatenate(turned, axis=0)), NT)
    for plane in range(2):
        for m in range(8):
            out_ref[pl.ds(plane * 8 + m, edge, stride=16), :] = lanes(last, m)[
                plane * edge : (plane + 1) * edge
            ]
    save.wait()


def strike_both(pencil, gain, past, tables):
    waves, twist = tables
    edge = twist.shape[1]
    modes = (2, 8, edge * edge)
    return pl.pallas_call(
        strike_kernel,
        out_shape=(
            jax.ShapeDtypeStruct(modes, F32),
            jax.ShapeDtypeStruct((edge * 16, edge), F32),
        ),
        in_specs=[VMEM, HBM, HBM, VMEM, VMEM],
        out_specs=(HBM, VMEM),
        scratch_shapes=[
            pltpu.VMEM(gain.shape, F32),
            pltpu.VMEM(past.shape, F32),
            pltpu.VMEM((2, edge * 8, edge), F32),
            pltpu.VMEM(modes, F32),
            pltpu.SemaphoreType.DMA((3,)),
        ],
        compiler_params=pltpu.CompilerParams(vmem_limit_bytes=WIDE),
        name="strike_both",
        cost_estimate=pl.CostEstimate(flops=1_600_000_000, bytes_accessed=6_000_000, transcendentals=0),
    )(pencil, *in_hbm(gain, past), waves, twist)


def past_kernel(kernel_ref, history_ref, gain_ref, past_ref):
    tiles = kernel_ref.shape[2] // 128
    for tile in range(tiles):
        cols = pl.ds(tile * 128, 128)
        rows = pl.ds(tile * 8, 8)
        gain_ref[rows, :] = kernel_ref[0, :, cols]
        for plane in range(2):
            total = kernel_ref[1, :, cols] * history_ref[0, plane, :, cols]
            for lag in range(1, LAGS):
                total = total + kernel_ref[lag + 1, :, cols] * history_ref[lag, plane, :, cols]
            past_ref[plane, rows, :] = total


def past_sum(kernel, history):
    length = kernel.shape[2]
    block = 2048
    return pl.pallas_call(
        past_kernel,
        grid=(length // block,),
        out_shape=(
            jax.ShapeDtypeStruct((length // 16, 128), F32),
            jax.ShapeDtypeStruct((2, length // 16, 128), F32),
        ),
        in_specs=[
            pl.BlockSpec((LAGS + 1, 8, block), lambda i: (0, 0, i)),
            pl.BlockSpec((LAGS, 2, 8, block), lambda i: (0, 0, 0, i)),
        ],
        out_specs=(
            pl.BlockSpec((block // 16, 128), lambda i: (i, 0)),
            pl.BlockSpec((2, block // 16, 128), lambda i: (0, i, 0)),
        ),
        compiler_params=pltpu.CompilerParams(vmem_limit_bytes=WIDE),
        name="past_sum",
        cost_estimate=pl.CostEstimate(flops=4_200_000, bytes_accessed=14_700_000, transcendentals=0),
    )(*in_hbm(kernel, history))


def newton_parts(rate, scaling, strength):
    scaled = rate * scaling
    magnitude = jnp.abs(scaled)
    square = 1.0 + scaled * scaled
    inverse = lax.rsqrt(square)
    positive = jnp.log(magnitude + square * inverse)
    friction = strength * jnp.where(scaled < 0, -positive, positive)
    return friction, 1.0 + (strength * scaling) * (inverse * (1.0 / DAMPING))


STEP = RELAXATION / DAMPING


def start_kernel(rate_ref, state_ref, weak_ref, strength_ref, stress_ref, scale_ref, rest_ref, gain_ref):
    scaling = 0.5 * jnp.exp(weak_ref[...] * state_ref[...])
    rate = rate_ref[...]
    friction, divisor = newton_parts(rate, scaling, strength_ref[...])
    gain = STEP / divisor
    scale_ref[...] = scaling
    gain_ref[...] = gain
    rest_ref[...] = rate + gain * (stress_ref[...] - DAMPING * rate - friction)


def friction_start(rate_prev, log_state, weakening, strength, pre_stress):
    rows, cells = rate_prev.shape
    spec = pl.BlockSpec((64, cells), lambda i: (i, 0))
    shape = jax.ShapeDtypeStruct((rows, cells), F32)
    return pl.pallas_call(
        start_kernel,
        grid=(rows // 64,),
        out_shape=(shape,) * 3,
        in_specs=[spec] * 5,
        out_specs=(spec,) * 3,
        compiler_params=pltpu.CompilerParams(vmem_limit_bytes=GRANT),
        name="friction_start",
        cost_estimate=pl.CostEstimate(flops=20_000_000, bytes_accessed=8_000_000, transcendentals=1_000_000),
    )(rate_prev, log_state, weakening, strength, pre_stress)


def friction_kernel(
    column, me_ref, own_ref, one_ref, two_ref, three_ref, scale_ref, rest_ref, gain_ref, strength_ref,
    stress_ref, slip_ref, *refs
):
    velocity_hbm, new_hbm, velocity_ref, new_ref, sems = refs[-5:]
    edge, width = own_ref.shape
    cols = pl.ds(column, width)
    saves = []
    for slot, ref in enumerate((own_ref, one_ref, two_ref, three_ref)):
        rows = pl.ds(pl.multiple_of((me_ref[0] ^ slot) * edge, edge), edge)
        elastic = ref[...]
        scaling, strength = scale_ref[rows, cols], strength_ref[rows, cols]
        total = stress_ref[rows, cols] + elastic
        rate = rest_ref[rows, cols] + gain_ref[rows, cols] * elastic
        for sweep in range(NEWTON_ITERS - 1):
            friction, divisor = newton_parts(rate, scaling, strength)
            rate = rate + STEP * (total - DAMPING * rate - friction) / divisor
        velocity_ref[slot] = rate
        new_ref[slot] = slip_ref[rows, cols] + ADVANCE * rate
        for n, (source, target) in enumerate(((velocity_ref, velocity_hbm), (new_ref, new_hbm))):
            save = pltpu.make_async_copy(source.at[slot], target.at[rows, cols], sems.at[slot, n])
            save.start()
            saves.append(save)
    for save in saves:
        save.wait()


def friction_finish(column, me, elastic, start, strength, pre_stress, fault_slip, held=()):
    edge, width = elastic[0].shape
    shape = jax.ShapeDtypeStruct(fault_slip.shape, F32)
    count = 1 + 4 + 6
    return pl.pallas_call(
        functools.partial(friction_kernel, column),
        in_specs=[SMEM] + [VMEM] * 10 + [HBM] * len(held),
        out_specs=(HBM, HBM),
        out_shape=(shape, shape),
        scratch_shapes=[
            pltpu.VMEM((4, edge, width), F32),
            pltpu.VMEM((4, edge, width), F32),
            pltpu.SemaphoreType.DMA((4, 2)),
        ],
        input_output_aliases={count + n: n for n in range(len(held))},
        compiler_params=pltpu.CompilerParams(vmem_limit_bytes=GRANT),
        name="friction_finish",
        cost_estimate=pl.CostEstimate(flops=20_000_000, bytes_accessed=5_000_000, transcendentals=1_000_000),
    )(me, *elastic, *start, strength, pre_stress, fault_slip, *in_hbm(*held))


def exchange(parts, size):
    swap = lambda part, k: lax.ppermute(part, "depth", [(place, place ^ k) for place in range(size)])
    moved = {k: swap(parts[k], k) for k in (2, 3, 1)}
    return [parts[0]] + [moved[k] for k in (1, 2, 3)]


def body(fault_slip, rate_prev, log_state, weakening, strength, pre_stress, kernel, history):
    rows, cells = fault_slip.shape
    depth_size = lax.axis_size("depth")
    devices = lax.axis_size("strike") * depth_size
    edge = rows // depth_size
    depth_len = cells * depth_size
    place = lax.axis_index("depth")
    me = place.reshape(1)
    lines, source = [], fault_slip
    for column, width in FORWARD:
        blocks = [
            lax.dynamic_slice(source, ((place ^ k) * edge, column), (edge, width))
            for k in range(depth_size)
        ]
        source, *blocks = lax.optimization_barrier((source, *blocks))
        lines.append(exchange(blocks, depth_size))
    tables = depth_tables(depth_len, devices)
    gain, past = past_sum(kernel, history)
    start = friction_start(rate_prev, log_state, weakening, strength, pre_stress)
    waves = None
    for (column, _), parts in zip(FORWARD, lines):
        waves = depth_forward(column, me, parts, tables, waves)
    pencil = lax.all_to_all(waves.reshape(devices, 16, edge), ALL, 0, 0)
    scale = 1.0 / math.sqrt(depth_len * edge * devices)
    slip_modes, waves = strike_both(
        pencil.reshape(devices * 16, edge), gain, past, strike_tables(edge, scale)
    )
    waves = lax.all_to_all(waves.reshape(devices, 16, edge), ALL, 0, 0).reshape(devices * 16, edge)
    elastic = [
        exchange(depth_inverse(column, width, me, waves, tables), depth_size)
        for column, width in INVERSE
    ]
    out = ()
    for (column, _), parts in zip(INVERSE, elastic):
        out = friction_finish(column, me, parts, start, strength, pre_stress, fault_slip, out)
    return (*out, slip_modes)


def solution(mesh):
    return jax.shard_map(
        body,
        mesh=mesh,
        in_specs=(
            P("strike", "depth"),
            P("strike", "depth"),
            P("strike", "depth"),
            P("strike", "depth"),
            P("strike", "depth"),
            P("strike", "depth"),
            P(None, ("strike", "depth"), None),
            P(None, None, ("strike", "depth"), None),
        ),
        out_specs=(P("strike", "depth"), P("strike", "depth"), P(None, ("strike", "depth"), None)),
        check_vma=False,
    )
```

```python
import functools
import math

import jax
import jax.numpy as jnp
import ml_dtypes
import numpy as np
from jax import lax
from jax.experimental import pallas as pl
from jax.experimental.pallas import tpu as pltpu
from jax.sharding import PartitionSpec as P

NEWTON_ITERS = 4
DAMPING = 0.5
RELAXATION = 0.5
ADVANCE = 0.5
LAGS = 8
FORWARD = ((0, 256), (256, 256))
INVERSE = ((0, 256), (256, 256))
SLOTS = (((0, 1, 2, 3),), ((0, 1), (2,), (3,)))
GRANT = 16 << 20
WIDE = 24 << 20
ALL = ("strike", "depth")
F32 = jnp.float32
BF16 = jnp.bfloat16
NN = (((1,), (0,)), ((), ()))
NT = (((1,), (1,)), ((), ()))
TN = (((0,), (0,)), ((), ()))
VMEM = pl.BlockSpec(memory_space=pltpu.VMEM)
SMEM = pl.BlockSpec(memory_space=pltpu.SMEM)
HBM = pl.BlockSpec(memory_space=pltpu.HBM)


def split_np(table):
    high = table.astype(ml_dtypes.bfloat16)
    low = (table - high.astype(np.float64)).astype(ml_dtypes.bfloat16)
    return high, low


def split(value):
    high = value.astype(BF16)
    return high, (value - high.astype(F32)).astype(BF16)


def in_hbm(*values):
    return [pltpu.with_memory_space_constraint(jnp.asarray(v), pltpu.HBM) for v in values]


def dot3(left, right, dims):
    (left_axis,), (right_axis,) = dims[0]
    return lax.dot_general(
        jnp.concatenate([left[0], left[0], left[1]], axis=left_axis),
        jnp.concatenate([right[0], right[1], right[0]], axis=right_axis),
        dims,
        preferred_element_type=F32,
    )


def depth_seeds(depth_len, blocks):
    cells = depth_len // 4
    cell = np.arange(cells)
    turn = 2.0 * np.pi / depth_len
    coarse = turn * ((8 * np.arange(blocks)[:, None] * cell[None]) % depth_len)
    fine = turn * ((np.arange(8)[:, None] * cell[None]) % depth_len)
    pack = lambda angle: np.stack([np.cos(angle), np.sin(angle)]).astype(np.float32)
    return pack(coarse), pack(fine)


def table_kernel(coarse_ref, fine_ref, high_ref, low_ref):
    blocks = coarse_ref.shape[1]
    cos_a, sin_a = coarse_ref[0], coarse_ref[1]
    for cls in range(4):
        for half in range(2):
            row = 4 * half + cls
            cos_b, sin_b = fine_ref[0, row : row + 1, :], fine_ref[1, row : row + 1, :]
            for part, value in enumerate(
                (cos_a * cos_b - sin_a * sin_b, sin_a * cos_b + cos_a * sin_b)
            ):
                high, low = split(value)
                rows = pl.ds((part * 2 + half) * blocks, blocks)
                high_ref[cls, rows, :] = high
                low_ref[cls, rows, :] = low


def depth_tables(depth_len, blocks):
    coarse, fine = depth_seeds(depth_len, blocks)
    shape = jax.ShapeDtypeStruct((4, 4 * blocks, depth_len // 4), BF16)
    return pl.pallas_call(
        table_kernel,
        out_shape=(shape, shape),
        in_specs=[VMEM, VMEM],
        out_specs=(VMEM, VMEM),
        compiler_params=pltpu.CompilerParams(vmem_limit_bytes=GRANT),
        name="depth_tables",
        cost_estimate=pl.CostEstimate(flops=10_000_000, bytes_accessed=5_000_000, transcendentals=0),
    )(coarse, fine)


def depth_forward_kernel(first, column, me_ref, own_ref, one_ref, two_ref, three_ref, high_ref, low_ref, *refs):
    rows, cells = own_ref.shape
    blocks = high_ref.shape[1] // 4
    cols = pl.ds(column, cells)
    me = me_ref[0]
    swap = (me & 1) == 1
    tau = (1 - 2 * (me & 1)).astype(F32)
    sigma = (1 - (me & 2)).astype(F32)
    even, odd = own_ref[...] + two_ref[...], one_ref[...] + three_ref[...]
    left, right = sigma * (own_ref[...] - two_ref[...]), sigma * (one_ref[...] - three_ref[...])
    both = jnp.concatenate(
        [jnp.where(swap, right, left), jnp.where(swap, left, right)], axis=0
    )

    def put(cls, real, imag):
        for plane, value in enumerate((real, imag)):
            for half in range(2):
                part = value[half * blocks : (half + 1) * blocks]
                slot = cls * 4 + plane * 2 + half
                if first:
                    refs[0][slot] = part
                else:
                    start = plane * 8 + half * 4 + cls
                    refs[1][pl.ds(start, blocks, stride=16), :] = part + refs[0][slot]

    def turn(cls, parts):
        return dot3((high_ref[cls, :, cols], low_ref[cls, :, cols]), parts, NT)

    top = 2 * blocks
    for cls, value in ((0, even + odd), (2, tau * (even - odd))):
        res = turn(cls, split(value))
        put(cls, res[:top], -res[top:])
    parts = split(both)
    res = turn(1, parts)
    put(1, res[:top, :rows] - res[top:, rows:], -(res[top:, :rows] + res[:top, rows:]))
    res = turn(3, parts)
    put(3, res[:top, :rows] + res[top:, rows:], res[:top, rows:] - res[top:, :rows])


def depth_forward(column, me, parts, tables, held=None):
    blocks = tables[0].shape[1] // 4
    rows = parts[0].shape[0]
    first = held is None
    shape = (16, blocks, rows) if first else (blocks * 16, rows)
    return pl.pallas_call(
        functools.partial(depth_forward_kernel, first, column),
        out_shape=jax.ShapeDtypeStruct(shape, F32),
        in_specs=[SMEM] + [VMEM] * (6 if first else 7),
        out_specs=VMEM,
        compiler_params=pltpu.CompilerParams(vmem_limit_bytes=GRANT),
        name="depth_forward",
        cost_estimate=pl.CostEstimate(flops=1_200_000_000, bytes_accessed=4_000_000, transcendentals=0),
    )(me, *parts, *tables, *(() if first else (held,)))


def depth_inverse_kernel(column, me_ref, y_ref, high_ref, low_ref, own_ref, one_ref, two_ref, three_ref):
    rows, cells = own_ref.shape
    blocks = high_ref.shape[1] // 4
    cols = pl.ds(column, cells)
    me = me_ref[0]
    swap = (me & 1) == 1
    tau = (1 - 2 * (me & 1)).astype(F32)
    sigma = (1 - (me & 2)).astype(F32)

    def get(cls, plane):
        return jnp.concatenate(
            [y_ref[pl.ds(plane * 8 + half * 4 + cls, blocks, stride=16), :] for half in range(2)],
            axis=0,
        )

    def turn(cls, value):
        return dot3(split(value), (high_ref[cls, :, cols], low_ref[cls, :, cols]), TN)

    real, imag = get(0, 0), get(0, 1)
    first = lax.broadcasted_iota(jnp.int32, real.shape, 0) == 0
    real = jnp.where(first, 0.5 * real, real)
    imag = jnp.where(first, 0.5 * imag, imag)
    zero = turn(0, jnp.concatenate([real, -imag], axis=0))
    two = tau * turn(2, jnp.concatenate([get(2, 0), -get(2, 1)], axis=0))
    real, imag = get(1, 0), get(1, 1)
    odd = turn(
        1,
        jnp.concatenate(
            [jnp.concatenate([real, -imag], axis=0), jnp.concatenate([-imag, -real], axis=0)], axis=1
        ),
    )
    real, imag = get(3, 0), get(3, 1)
    odd = sigma * (
        odd
        + turn(
            3,
            jnp.concatenate(
                [jnp.concatenate([real, -imag], axis=0), jnp.concatenate([imag, real], axis=0)], axis=1
            ),
        )
    )
    low, high = odd[:rows], odd[rows:]
    base, turned = zero + two, jnp.where(swap, high, low)
    own_ref[...] = base + turned
    two_ref[...] = base - turned
    base, turned = zero - two, jnp.where(swap, low, high)
    one_ref[...] = base + turned
    three_ref[...] = base - turned


def depth_inverse(column, width, me, waves, tables):
    rows = waves.shape[1]
    shape = jax.ShapeDtypeStruct((rows, width), F32)
    return pl.pallas_call(
        functools.partial(depth_inverse_kernel, column),
        out_shape=(shape,) * 4,
        in_specs=[SMEM] + [VMEM] * 3,
        out_specs=(VMEM,) * 4,
        compiler_params=pltpu.CompilerParams(vmem_limit_bytes=GRANT),
        name="depth_inverse",
        cost_estimate=pl.CostEstimate(flops=1_200_000_000, bytes_accessed=4_000_000, transcendentals=0),
    )(me, waves, *tables)


def strike_tables(edge, scale):
    turn = 2.0 * np.pi / edge
    angle = turn * (np.outer(np.arange(edge), np.arange(edge)) % edge)
    waves = np.stack([*split_np(np.cos(angle)), *split_np(np.sin(angle))])
    twist = 2.0 * np.pi / (edge * edge) * np.outer(np.arange(edge), np.arange(edge))
    twist = np.stack([np.cos(twist), np.sin(twist)]) * scale
    return waves, twist.astype(np.float32)


def strike_kernel(
    x_ref, gain_hbm, past_hbm, wave_ref, twist_ref, modes_hbm, out_ref,
    gain_ref, past_ref, modes_ref, sems,
):
    edge = twist_ref.shape[1]
    pairs = ((gain_hbm, gain_ref), (past_hbm, past_ref))
    loads = [pltpu.make_async_copy(a, b, sems.at[n]) for n, (a, b) in enumerate(pairs)]
    for load in loads:
        load.start()
    lanes = lambda value, m: value[:, m * edge : (m + 1) * edge]

    def gather(ref, m):
        return jnp.concatenate(
            [ref[pl.ds(plane * 8 + m, edge, stride=16), :] for plane in range(2)], axis=0
        )

    parts = split(jnp.concatenate([gather(x_ref, m) for m in range(8)], axis=1))

    def block(sign, part):
        cosine, sine = wave_ref[part], wave_ref[2 + part]
        left, right = (sine, -sine) if sign > 0 else (-sine, sine)
        return jnp.concatenate(
            [jnp.concatenate([cosine, left], axis=1), jnp.concatenate([right, cosine], axis=1)], axis=0
        )

    forward = (block(1, 0), block(1, 1))
    backward = (block(-1, 0), block(-1, 1))
    first = dot3(forward, parts, NN)
    cosine, sine = twist_ref[0], twist_ref[1]
    turned = []
    for m in range(8):
        part = lanes(first, m)
        real, imag = part[:edge], part[edge:]
        turned.append(
            jnp.concatenate([real * cosine + imag * sine, imag * cosine - real * sine], axis=1)
        )
    modes = dot3(forward, split(jnp.concatenate(turned, axis=0)), NT)
    for plane in range(2):
        for m in range(8):
            modes_ref[plane, pl.ds(m, edge, stride=8), :] = lanes(modes, m)[
                plane * edge : (plane + 1) * edge
            ]
    save = pltpu.make_async_copy(modes_ref, modes_hbm, sems.at[2])
    save.start()
    for load in loads:
        load.wait()
    spectrum = []
    for m in range(8):
        part, gain = lanes(modes, m), gain_ref[m]
        spectrum.append(
            jnp.concatenate(
                [gain * part[:edge] + past_ref[0, m], gain * part[edge:] + past_ref[1, m]], axis=0
            )
        )
    third = dot3(backward, split(jnp.concatenate(spectrum, axis=1)), NN)
    turned = []
    for m in range(8):
        part = lanes(third, m)
        real, imag = part[:edge], part[edge:]
        turned.append(
            jnp.concatenate(
                [2.0 * (real * cosine - imag * sine), 2.0 * (imag * cosine + real * sine)], axis=1
            )
        )
    last = dot3(backward, split(jnp.concatenate(turned, axis=0)), NT)
    for plane in range(2):
        for m in range(8):
            out_ref[pl.ds(plane * 8 + m, edge, stride=16), :] = lanes(last, m)[
                plane * edge : (plane + 1) * edge
            ]
    save.wait()


def strike_both(pencil, gain, past, tables):
    waves, twist = tables
    edge = twist.shape[1]
    modes = (2, edge * 8, edge)
    return pl.pallas_call(
        strike_kernel,
        out_shape=(
            pltpu.HBM(modes, F32),
            jax.ShapeDtypeStruct((edge * 16, edge), F32),
        ),
        in_specs=[VMEM, HBM, HBM, VMEM, VMEM],
        out_specs=(HBM, VMEM),
        scratch_shapes=[
            pltpu.VMEM(gain.shape, F32),
            pltpu.VMEM(past.shape, F32),
            pltpu.VMEM(modes, F32),
            pltpu.SemaphoreType.DMA((3,)),
        ],
        compiler_params=pltpu.CompilerParams(vmem_limit_bytes=WIDE),
        name="strike_both",
        cost_estimate=pl.CostEstimate(flops=1_600_000_000, bytes_accessed=6_000_000, transcendentals=0),
    )(pencil, *in_hbm(gain, past), waves, twist)


def past_kernel(kernel_ref, history_ref, gain_ref, past_ref):
    for tile in range(kernel_ref.shape[2] // 128):
        cols = pl.ds(tile * 128, 128)
        gain_ref[:, tile, :] = kernel_ref[0, :, cols]
        for plane in range(2):
            total = kernel_ref[1, :, cols] * history_ref[0, plane, :, cols]
            for lag in range(1, LAGS):
                total = total + kernel_ref[lag + 1, :, cols] * history_ref[lag, plane, :, cols]
            past_ref[plane, :, tile, :] = total


def past_sum(kernel, history):
    length = kernel.shape[2]
    block = 2048
    return pl.pallas_call(
        past_kernel,
        grid=(length // block,),
        out_shape=(
            pltpu.HBM((8, length // 128, 128), F32),
            pltpu.HBM((2, 8, length // 128, 128), F32),
        ),
        in_specs=[
            pl.BlockSpec((LAGS + 1, 8, block), lambda i: (0, 0, i)),
            pl.BlockSpec((LAGS, 2, 8, block), lambda i: (0, 0, 0, i)),
        ],
        out_specs=(
            pl.BlockSpec((8, block // 128, 128), lambda i: (0, i, 0)),
            pl.BlockSpec((2, 8, block // 128, 128), lambda i: (0, 0, i, 0)),
        ),
        compiler_params=pltpu.CompilerParams(vmem_limit_bytes=WIDE),
        name="past_sum",
        cost_estimate=pl.CostEstimate(flops=4_200_000, bytes_accessed=14_700_000, transcendentals=0),
    )(*in_hbm(kernel, history))


def newton_parts(rate, scaling, strength):
    scaled = rate * scaling
    magnitude = jnp.abs(scaled)
    square = 1.0 + scaled * scaled
    inverse = lax.rsqrt(square)
    positive = jnp.log(magnitude + square * inverse)
    friction = strength * jnp.where(scaled < 0, -positive, positive)
    return friction, 1.0 + (strength * scaling) * (inverse * (1.0 / DAMPING))


STEP = RELAXATION / DAMPING


def start_kernel(rate_ref, state_ref, weak_ref, strength_ref, stress_ref, scale_ref, rest_ref, gain_ref):
    scaling = 0.5 * jnp.exp(weak_ref[...] * state_ref[...])
    rate = rate_ref[...]
    friction, divisor = newton_parts(rate, scaling, strength_ref[...])
    gain = STEP / divisor
    scale_ref[...] = scaling
    gain_ref[...] = gain
    rest_ref[...] = rate + gain * (stress_ref[...] - DAMPING * rate - friction)


def friction_start(rate_prev, log_state, weakening, strength, pre_stress):
    rows, cells = rate_prev.shape
    spec = pl.BlockSpec((64, cells), lambda i: (i, 0))
    shape = jax.ShapeDtypeStruct((rows, cells), F32)
    return pl.pallas_call(
        start_kernel,
        grid=(rows // 64,),
        out_shape=(shape,) * 3,
        in_specs=[spec] * 5,
        out_specs=(spec,) * 3,
        compiler_params=pltpu.CompilerParams(vmem_limit_bytes=GRANT),
        name="friction_start",
        cost_estimate=pl.CostEstimate(flops=20_000_000, bytes_accessed=8_000_000, transcendentals=1_000_000),
    )(rate_prev, log_state, weakening, strength, pre_stress)


def friction_kernel(
    slots, column, me_ref, scale_ref, rest_ref, gain_ref, strength_ref, stress_ref, slip_ref, *refs
):
    velocity_hbm, new_hbm, velocity_ref, new_ref, sems = refs[-5:]
    parts = refs[: len(slots)]
    edge, width = parts[0].shape
    cols = pl.ds(column, width)
    saves = []
    for place, (slot, ref) in enumerate(zip(slots, parts)):
        rows = pl.ds(pl.multiple_of((me_ref[0] ^ slot) * edge, edge), edge)
        elastic = ref[...]
        scaling, strength = scale_ref[rows, cols], strength_ref[rows, cols]
        total = stress_ref[rows, cols] + elastic
        rate = rest_ref[rows, cols] + gain_ref[rows, cols] * elastic
        for sweep in range(NEWTON_ITERS - 1):
            friction, divisor = newton_parts(rate, scaling, strength)
            rate = rate + STEP * (total - DAMPING * rate - friction) / divisor
        velocity_ref[place] = rate
        new_ref[place] = slip_ref[rows, cols] + ADVANCE * rate
        for n, (source, target) in enumerate(((velocity_ref, velocity_hbm), (new_ref, new_hbm))):
            save = pltpu.make_async_copy(source.at[place], target.at[rows, cols], sems.at[place, n])
            save.start()
            saves.append(save)
    for save in saves:
        save.wait()


def friction_finish(slots, column, me, elastic, start, strength, pre_stress, fault_slip, held=()):
    edge, width = elastic[0].shape
    shape = jax.ShapeDtypeStruct(fault_slip.shape, F32)
    count = 7 + len(slots)
    return pl.pallas_call(
        functools.partial(friction_kernel, slots, column),
        in_specs=[SMEM] + [VMEM] * (6 + len(slots)) + [HBM] * len(held),
        out_specs=(HBM, HBM),
        out_shape=(shape, shape),
        scratch_shapes=[
            pltpu.VMEM((len(slots), edge, width), F32),
            pltpu.VMEM((len(slots), edge, width), F32),
            pltpu.SemaphoreType.DMA((len(slots), 2)),
        ],
        input_output_aliases={count + n: n for n in range(len(held))},
        compiler_params=pltpu.CompilerParams(vmem_limit_bytes=GRANT),
        name="friction_finish",
        cost_estimate=pl.CostEstimate(flops=20_000_000, bytes_accessed=5_000_000, transcendentals=1_000_000),
    )(me, *start, strength, pre_stress, fault_slip, *elastic, *in_hbm(*held))


def exchange(parts, size):
    swap = lambda part, k: lax.ppermute(part, "depth", [(place, place ^ k) for place in range(size)])
    moved = {k: swap(parts[k], k) for k in (2, 3, 1)}
    return [parts[0]] + [moved[k] for k in (1, 2, 3)]


def body(fault_slip, rate_prev, log_state, weakening, strength, pre_stress, kernel, history):
    rows, cells = fault_slip.shape
    depth_size = lax.axis_size("depth")
    devices = lax.axis_size("strike") * depth_size
    edge = rows // depth_size
    depth_len = cells * depth_size
    place = lax.axis_index("depth")
    me = place.reshape(1)
    lines, source = [], fault_slip
    for column, width in FORWARD:
        blocks = [
            lax.dynamic_slice(source, ((place ^ k) * edge, column), (edge, width))
            for k in range(depth_size)
        ]
        source, *blocks = lax.optimization_barrier((source, *blocks))
        lines.append(exchange(blocks, depth_size))
    tables = depth_tables(depth_len, devices)
    gain, past = past_sum(kernel, history)
    waves = None
    for (column, _), parts in zip(FORWARD, lines):
        waves = depth_forward(column, me, parts, tables, waves)
    pencil = lax.all_to_all(waves.reshape(devices, 16, edge), ALL, 0, 0)
    scale = 1.0 / math.sqrt(depth_len * edge * devices)
    modes, waves = strike_both(
        pencil.reshape(devices * 16, edge), gain, past, strike_tables(edge, scale)
    )
    start = friction_start(rate_prev, log_state, weakening, strength, pre_stress)
    waves = lax.all_to_all(waves.reshape(devices, 16, edge), ALL, 0, 0).reshape(devices * 16, edge)
    elastic = [
        exchange(depth_inverse(column, width, me, waves, tables), depth_size)
        for column, width in INVERSE
    ]
    out = ()
    for (column, _), parts, groups in zip(INVERSE, elastic, SLOTS):
        for slots in groups:
            parts_now = [parts[slot] for slot in slots]
            out = friction_finish(
                slots, column, me, parts_now, start, strength, pre_stress, fault_slip, out
            )
    slip_modes = modes.reshape(2, devices, 8, edge).transpose(0, 2, 1, 3).reshape(2, 8, devices * edge)
    return (*out, slip_modes)


def solution(mesh):
    return jax.shard_map(
        body,
        mesh=mesh,
        in_specs=(
            P("strike", "depth"),
            P("strike", "depth"),
            P("strike", "depth"),
            P("strike", "depth"),
            P("strike", "depth"),
            P("strike", "depth"),
            P(None, ("strike", "depth"), None),
            P(None, None, ("strike", "depth"), None),
        ),
        out_specs=(P("strike", "depth"), P("strike", "depth"), P(None, ("strike", "depth"), None)),
        check_vma=False,
    )
```

```python
import functools
import math

import jax
import jax.numpy as jnp
import ml_dtypes
import numpy as np
from jax import lax
from jax.experimental import pallas as pl
from jax.experimental.pallas import tpu as pltpu
from jax.sharding import PartitionSpec as P

NEWTON_ITERS = 4
DAMPING = 0.5
RELAXATION = 0.5
ADVANCE = 0.5
LAGS = 8
FORWARD = ((0, 256), (256, 256))
INVERSE = ((0, 256), (256, 256))
SLOTS = (((0, 1, 2, 3),), ((0, 1), (2,), (3,)))
PAIR = 2
GRANT = 16 << 20
WIDE = 24 << 20
ALL = ("strike", "depth")
F32 = jnp.float32
BF16 = jnp.bfloat16
NN = (((1,), (0,)), ((), ()))
NT = (((1,), (1,)), ((), ()))
TN = (((0,), (0,)), ((), ()))
VMEM = pl.BlockSpec(memory_space=pltpu.VMEM)
SMEM = pl.BlockSpec(memory_space=pltpu.SMEM)
HBM = pl.BlockSpec(memory_space=pltpu.HBM)


def split_np(table):
    high = table.astype(ml_dtypes.bfloat16)
    low = (table - high.astype(np.float64)).astype(ml_dtypes.bfloat16)
    return high, low


def split(value):
    high = value.astype(BF16)
    return high, (value - high.astype(F32)).astype(BF16)


def in_hbm(*values):
    return [pltpu.with_memory_space_constraint(jnp.asarray(v), pltpu.HBM) for v in values]


def dot3(left, right, dims):
    (left_axis,), (right_axis,) = dims[0]
    return lax.dot_general(
        jnp.concatenate([left[0], left[0], left[1]], axis=left_axis),
        jnp.concatenate([right[0], right[1], right[0]], axis=right_axis),
        dims,
        preferred_element_type=F32,
    )


def depth_seeds(depth_len, blocks):
    cells = depth_len // 4
    cell = np.arange(cells)
    turn = 2.0 * np.pi / depth_len
    coarse = turn * ((8 * np.arange(blocks)[:, None] * cell[None]) % depth_len)
    fine = turn * ((np.arange(8)[:, None] * cell[None]) % depth_len)
    pack = lambda angle: np.stack([np.cos(angle), np.sin(angle)]).astype(np.float32)
    return pack(coarse), pack(fine)


def table_kernel(coarse_ref, fine_ref, high_ref, low_ref):
    blocks = coarse_ref.shape[1]
    cos_a, sin_a = coarse_ref[0], coarse_ref[1]
    for cls in range(4):
        for half in range(2):
            row = 4 * half + cls
            cos_b, sin_b = fine_ref[0, row : row + 1, :], fine_ref[1, row : row + 1, :]
            for part, value in enumerate(
                (cos_a * cos_b - sin_a * sin_b, sin_a * cos_b + cos_a * sin_b)
            ):
                high, low = split(value)
                rows = pl.ds((part * 2 + half) * blocks, blocks)
                high_ref[cls, rows, :] = high
                low_ref[cls, rows, :] = low


def depth_tables(depth_len, blocks):
    coarse, fine = depth_seeds(depth_len, blocks)
    shape = jax.ShapeDtypeStruct((4, 4 * blocks, depth_len // 4), BF16)
    return pl.pallas_call(
        table_kernel,
        out_shape=(shape, shape),
        in_specs=[VMEM, VMEM],
        out_specs=(VMEM, VMEM),
        compiler_params=pltpu.CompilerParams(vmem_limit_bytes=GRANT),
        name="depth_tables",
        cost_estimate=pl.CostEstimate(flops=10_000_000, bytes_accessed=5_000_000, transcendentals=0),
    )(coarse, fine)


def depth_forward_kernel(first, column, me_ref, own_ref, one_ref, two_ref, three_ref, high_ref, low_ref, *refs):
    rows, cells = own_ref.shape
    blocks = high_ref.shape[1] // 4
    cols = pl.ds(column, cells)
    me = me_ref[0]
    swap = (me & 1) == 1
    tau = (1 - 2 * (me & 1)).astype(F32)
    sigma = (1 - (me & 2)).astype(F32)
    even, odd = own_ref[...] + two_ref[...], one_ref[...] + three_ref[...]
    left, right = sigma * (own_ref[...] - two_ref[...]), sigma * (one_ref[...] - three_ref[...])
    both = jnp.concatenate(
        [jnp.where(swap, right, left), jnp.where(swap, left, right)], axis=0
    )

    def put(cls, real, imag):
        for plane, value in enumerate((real, imag)):
            for half in range(2):
                part = value[half * blocks : (half + 1) * blocks]
                slot = cls * 4 + plane * 2 + half
                if first:
                    refs[0][slot] = part
                else:
                    start = plane * 8 + half * 4 + cls
                    refs[1][pl.ds(start, blocks, stride=16), :] = part + refs[0][slot]

    def turn(cls, parts):
        return dot3((high_ref[cls, :, cols], low_ref[cls, :, cols]), parts, NT)

    top = 2 * blocks
    for cls, value in ((0, even + odd), (2, tau * (even - odd))):
        res = turn(cls, split(value))
        put(cls, res[:top], -res[top:])
    parts = split(both)
    res = turn(1, parts)
    put(1, res[:top, :rows] - res[top:, rows:], -(res[top:, :rows] + res[:top, rows:]))
    res = turn(3, parts)
    put(3, res[:top, :rows] + res[top:, rows:], res[:top, rows:] - res[top:, :rows])


def depth_forward(column, me, parts, tables, held=None):
    blocks = tables[0].shape[1] // 4
    rows = parts[0].shape[0]
    first = held is None
    shape = (16, blocks, rows) if first else (blocks * 16, rows)
    return pl.pallas_call(
        functools.partial(depth_forward_kernel, first, column),
        out_shape=jax.ShapeDtypeStruct(shape, F32),
        in_specs=[SMEM] + [VMEM] * (6 if first else 7),
        out_specs=VMEM,
        compiler_params=pltpu.CompilerParams(vmem_limit_bytes=GRANT),
        name="depth_forward",
        cost_estimate=pl.CostEstimate(flops=1_200_000_000, bytes_accessed=4_000_000, transcendentals=0),
    )(me, *parts, *tables, *(() if first else (held,)))


def depth_inverse_kernel(column, me_ref, y_ref, high_ref, low_ref, own_ref, one_ref, two_ref, three_ref):
    rows, cells = own_ref.shape
    blocks = high_ref.shape[1] // 4
    cols = pl.ds(column, cells)
    me = me_ref[0]
    swap = (me & 1) == 1
    tau = (1 - 2 * (me & 1)).astype(F32)
    sigma = (1 - (me & 2)).astype(F32)

    def get(cls, plane):
        return jnp.concatenate(
            [y_ref[pl.ds(plane * 8 + half * 4 + cls, blocks, stride=16), :] for half in range(2)],
            axis=0,
        )

    def turn(cls, value):
        return dot3(split(value), (high_ref[cls, :, cols], low_ref[cls, :, cols]), TN)

    real, imag = get(0, 0), get(0, 1)
    first = lax.broadcasted_iota(jnp.int32, real.shape, 0) == 0
    real = jnp.where(first, 0.5 * real, real)
    imag = jnp.where(first, 0.5 * imag, imag)
    zero = turn(0, jnp.concatenate([real, -imag], axis=0))
    two = tau * turn(2, jnp.concatenate([get(2, 0), -get(2, 1)], axis=0))
    real, imag = get(1, 0), get(1, 1)
    odd = turn(
        1,
        jnp.concatenate(
            [jnp.concatenate([real, -imag], axis=0), jnp.concatenate([-imag, -real], axis=0)], axis=1
        ),
    )
    real, imag = get(3, 0), get(3, 1)
    odd = sigma * (
        odd
        + turn(
            3,
            jnp.concatenate(
                [jnp.concatenate([real, -imag], axis=0), jnp.concatenate([imag, real], axis=0)], axis=1
            ),
        )
    )
    low, high = odd[:rows], odd[rows:]
    base, turned = zero + two, jnp.where(swap, high, low)
    own_ref[...] = base + turned
    two_ref[...] = base - turned
    base, turned = zero - two, jnp.where(swap, low, high)
    one_ref[...] = base + turned
    three_ref[...] = base - turned


def depth_inverse(column, width, me, waves, tables):
    rows = waves.shape[1]
    shape = jax.ShapeDtypeStruct((rows, width), F32)
    return pl.pallas_call(
        functools.partial(depth_inverse_kernel, column),
        out_shape=(shape,) * 4,
        in_specs=[SMEM] + [VMEM] * 3,
        out_specs=(VMEM,) * 4,
        compiler_params=pltpu.CompilerParams(vmem_limit_bytes=GRANT),
        name="depth_inverse",
        cost_estimate=pl.CostEstimate(flops=1_200_000_000, bytes_accessed=4_000_000, transcendentals=0),
    )(me, waves, *tables)


def strike_tables(edge, scale):
    turn = 2.0 * np.pi / edge
    angle = turn * (np.outer(np.arange(edge), np.arange(edge)) % edge)
    waves = np.stack([*split_np(np.cos(angle)), *split_np(np.sin(angle))])
    twist = 2.0 * np.pi / (edge * edge) * np.outer(np.arange(edge), np.arange(edge))
    twist = np.stack([np.cos(twist), np.sin(twist)]) * scale
    return waves, np.concatenate([twist, 2.0 * twist]).astype(np.float32)


def strike_kernel(
    x_ref, gain_hbm, past_hbm, wave_ref, twist_ref, modes_hbm, out_ref,
    gain_ref, past_ref, held_ref, modes_ref, sems,
):
    edge = twist_ref.shape[1]
    pairs = ((gain_hbm, gain_ref), (past_hbm, past_ref))
    loads = [pltpu.make_async_copy(a, b, sems.at[n]) for n, (a, b) in enumerate(pairs)]
    for load in loads:
        load.start()

    def lines(group):
        return range(group * PAIR, (group + 1) * PAIR)

    def lanes(value, place):
        part = value[:, place * edge : (place + 1) * edge]
        return part[:edge], part[edge:]

    def gather(m):
        return jnp.concatenate(
            [x_ref[pl.ds(plane * 8 + m, edge, stride=16), :] for plane in range(2)], axis=0
        )

    def block(sign, part):
        cosine, sine = wave_ref[part], wave_ref[2 + part]
        left, right = (sine, -sine) if sign > 0 else (-sine, sine)
        return jnp.concatenate(
            [jnp.concatenate([cosine, left], axis=1), jnp.concatenate([right, cosine], axis=1)], axis=0
        )

    def rotate(value, sign, cosine, sine):
        rows = []
        for place in range(PAIR):
            real, imag = lanes(value, place)
            if sign > 0:
                rows.append([real * cosine + imag * sine, imag * cosine - real * sine])
            else:
                rows.append([real * cosine - imag * sine, imag * cosine + real * sine])
        return jnp.concatenate([jnp.concatenate(row, axis=1) for row in rows], axis=0)

    forward = (block(1, 0), block(1, 1))
    for group in range(8 // PAIR):
        value = jnp.concatenate([gather(m) for m in lines(group)], axis=1)
        value = dot3(forward, split(value), NN)
        value = dot3(forward, split(rotate(value, 1, twist_ref[0], twist_ref[1])), NT)
        for place, m in enumerate(lines(group)):
            for plane, part in enumerate(lanes(value, place)):
                held_ref[plane, m] = part
                modes_ref[plane, pl.ds(m, edge, stride=8), :] = part
    save = pltpu.make_async_copy(modes_ref, modes_hbm, sems.at[2])
    save.start()
    for load in loads:
        load.wait()
    backward = (block(-1, 0), block(-1, 1))
    for group in range(8 // PAIR):
        value = jnp.concatenate(
            [
                jnp.concatenate(
                    [gain_ref[m] * held_ref[plane, m] + past_ref[plane, m] for plane in range(2)], axis=0
                )
                for m in lines(group)
            ],
            axis=1,
        )
        value = dot3(backward, split(value), NN)
        value = dot3(backward, split(rotate(value, -1, twist_ref[2], twist_ref[3])), NT)
        for place, m in enumerate(lines(group)):
            for plane, part in enumerate(lanes(value, place)):
                out_ref[pl.ds(plane * 8 + m, edge, stride=16), :] = part
    save.wait()


def strike_both(pencil, gain, past, tables):
    waves, twist = tables
    edge = twist.shape[1]
    modes = (2, edge * 8, edge)
    return pl.pallas_call(
        strike_kernel,
        out_shape=(
            pltpu.HBM(modes, F32),
            jax.ShapeDtypeStruct((edge * 16, edge), F32),
        ),
        in_specs=[VMEM, HBM, HBM, VMEM, VMEM],
        out_specs=(HBM, VMEM),
        scratch_shapes=[
            pltpu.VMEM(gain.shape, F32),
            pltpu.VMEM(past.shape, F32),
            pltpu.VMEM(past.shape, F32),
            pltpu.VMEM(modes, F32),
            pltpu.SemaphoreType.DMA((3,)),
        ],
        compiler_params=pltpu.CompilerParams(vmem_limit_bytes=WIDE),
        name="strike_both",
        cost_estimate=pl.CostEstimate(flops=1_600_000_000, bytes_accessed=6_000_000, transcendentals=0),
    )(pencil, *in_hbm(gain, past), waves, twist)


def past_kernel(kernel_ref, history_ref, gain_ref, past_ref):
    for tile in range(kernel_ref.shape[2] // 128):
        cols = pl.ds(tile * 128, 128)
        gain_ref[:, tile, :] = kernel_ref[0, :, cols]
        for plane in range(2):
            total = kernel_ref[1, :, cols] * history_ref[0, plane, :, cols]
            for lag in range(1, LAGS):
                total = total + kernel_ref[lag + 1, :, cols] * history_ref[lag, plane, :, cols]
            past_ref[plane, :, tile, :] = total


def past_sum(kernel, history):
    length = kernel.shape[2]
    block = 2048
    return pl.pallas_call(
        past_kernel,
        grid=(length // block,),
        out_shape=(
            pltpu.HBM((8, length // 128, 128), F32),
            pltpu.HBM((2, 8, length // 128, 128), F32),
        ),
        in_specs=[
            pl.BlockSpec((LAGS + 1, 8, block), lambda i: (0, 0, i)),
            pl.BlockSpec((LAGS, 2, 8, block), lambda i: (0, 0, 0, i)),
        ],
        out_specs=(
            pl.BlockSpec((8, block // 128, 128), lambda i: (0, i, 0)),
            pl.BlockSpec((2, 8, block // 128, 128), lambda i: (0, 0, i, 0)),
        ),
        compiler_params=pltpu.CompilerParams(vmem_limit_bytes=WIDE),
        name="past_sum",
        cost_estimate=pl.CostEstimate(flops=4_200_000, bytes_accessed=14_700_000, transcendentals=0),
    )(*in_hbm(kernel, history))


def newton_parts(rate, scaling, strength):
    scaled = rate * scaling
    magnitude = jnp.abs(scaled)
    square = 1.0 + scaled * scaled
    inverse = lax.rsqrt(square)
    positive = jnp.log(magnitude + square * inverse)
    friction = strength * jnp.where(scaled < 0, -positive, positive)
    return friction, 1.0 + (strength * scaling) * (inverse * (1.0 / DAMPING))


STEP = RELAXATION / DAMPING


def start_kernel(rate_ref, state_ref, weak_ref, strength_ref, stress_ref, scale_ref, rest_ref, gain_ref):
    scaling = 0.5 * jnp.exp(weak_ref[...] * state_ref[...])
    rate = rate_ref[...]
    friction, divisor = newton_parts(rate, scaling, strength_ref[...])
    gain = STEP / divisor
    scale_ref[...] = scaling
    gain_ref[...] = gain
    rest_ref[...] = rate + gain * (stress_ref[...] - DAMPING * rate - friction)


def friction_start(rate_prev, log_state, weakening, strength, pre_stress):
    rows, cells = rate_prev.shape
    spec = pl.BlockSpec((64, cells), lambda i: (i, 0))
    shape = jax.ShapeDtypeStruct((rows, cells), F32)
    return pl.pallas_call(
        start_kernel,
        grid=(rows // 64,),
        out_shape=(shape,) * 3,
        in_specs=[spec] * 5,
        out_specs=(spec,) * 3,
        compiler_params=pltpu.CompilerParams(vmem_limit_bytes=GRANT),
        name="friction_start",
        cost_estimate=pl.CostEstimate(flops=20_000_000, bytes_accessed=8_000_000, transcendentals=1_000_000),
    )(rate_prev, log_state, weakening, strength, pre_stress)


def friction_kernel(
    slots, column, me_ref, scale_ref, rest_ref, gain_ref, strength_ref, stress_ref, slip_ref, *refs
):
    velocity_hbm, new_hbm, velocity_ref, new_ref, sems = refs[-5:]
    parts = refs[: len(slots)]
    edge, width = parts[0].shape
    cols = pl.ds(column, width)
    saves = []
    for place, (slot, ref) in enumerate(zip(slots, parts)):
        rows = pl.ds(pl.multiple_of((me_ref[0] ^ slot) * edge, edge), edge)
        elastic = ref[...]
        scaling, strength = scale_ref[rows, cols], strength_ref[rows, cols]
        total = stress_ref[rows, cols] + elastic
        rate = rest_ref[rows, cols] + gain_ref[rows, cols] * elastic
        for sweep in range(NEWTON_ITERS - 1):
            friction, divisor = newton_parts(rate, scaling, strength)
            rate = rate + STEP * (total - DAMPING * rate - friction) / divisor
        velocity_ref[place] = rate
        new_ref[place] = slip_ref[rows, cols] + ADVANCE * rate
        for n, (source, target) in enumerate(((velocity_ref, velocity_hbm), (new_ref, new_hbm))):
            save = pltpu.make_async_copy(source.at[place], target.at[rows, cols], sems.at[place, n])
            save.start()
            saves.append(save)
    for save in saves:
        save.wait()


def friction_finish(slots, column, me, elastic, start, strength, pre_stress, fault_slip, held=()):
    edge, width = elastic[0].shape
    shape = jax.ShapeDtypeStruct(fault_slip.shape, F32)
    count = 7 + len(slots)
    return pl.pallas_call(
        functools.partial(friction_kernel, slots, column),
        in_specs=[SMEM] + [VMEM] * (6 + len(slots)) + [HBM] * len(held),
        out_specs=(HBM, HBM),
        out_shape=(shape, shape),
        scratch_shapes=[
            pltpu.VMEM((len(slots), edge, width), F32),
            pltpu.VMEM((len(slots), edge, width), F32),
            pltpu.SemaphoreType.DMA((len(slots), 2)),
        ],
        input_output_aliases={count + n: n for n in range(len(held))},
        compiler_params=pltpu.CompilerParams(vmem_limit_bytes=GRANT),
        name="friction_finish",
        cost_estimate=pl.CostEstimate(flops=20_000_000, bytes_accessed=5_000_000, transcendentals=1_000_000),
    )(me, *start, strength, pre_stress, fault_slip, *elastic, *in_hbm(*held))


def exchange(parts, size):
    swap = lambda part, k: lax.ppermute(part, "depth", [(place, place ^ k) for place in range(size)])
    moved = {k: swap(parts[k], k) for k in (2, 3, 1)}
    return [parts[0]] + [moved[k] for k in (1, 2, 3)]


def body(fault_slip, rate_prev, log_state, weakening, strength, pre_stress, kernel, history):
    rows, cells = fault_slip.shape
    depth_size = lax.axis_size("depth")
    devices = lax.axis_size("strike") * depth_size
    edge = rows // depth_size
    depth_len = cells * depth_size
    place = lax.axis_index("depth")
    me = place.reshape(1)
    block = lambda source, k, part: lax.dynamic_slice(
        source, ((place ^ k) * edge, part[0]), (edge, part[1])
    )
    far = [block(fault_slip, k, FORWARD[0]) for k in (2, 3)]
    source, *far = lax.optimization_barrier((fault_slip, *far))
    near = [block(source, k, FORWARD[0]) for k in (0, 1)]
    lines = [exchange(near + far, depth_size)]
    for part in FORWARD[1:]:
        lines.append(exchange([block(source, k, part) for k in range(depth_size)], depth_size))
    tables = depth_tables(depth_len, devices)
    gain, past = past_sum(kernel, history)
    waves = None
    for (column, _), parts in zip(FORWARD, lines):
        waves = depth_forward(column, me, parts, tables, waves)
    pencil = lax.all_to_all(waves.reshape(devices, 16, edge), ALL, 0, 0)
    scale = 1.0 / math.sqrt(depth_len * edge * devices)
    modes, waves = strike_both(
        pencil.reshape(devices * 16, edge), gain, past, strike_tables(edge, scale)
    )
    start = friction_start(rate_prev, log_state, weakening, strength, pre_stress)
    waves = lax.all_to_all(waves.reshape(devices, 16, edge), ALL, 0, 0).reshape(devices * 16, edge)
    elastic = [
        exchange(depth_inverse(column, width, me, waves, tables), depth_size)
        for column, width in INVERSE
    ]
    out = ()
    for (column, _), parts, groups in zip(INVERSE, elastic, SLOTS):
        for slots in groups:
            parts_now = [parts[slot] for slot in slots]
            out = friction_finish(
                slots, column, me, parts_now, start, strength, pre_stress, fault_slip, out
            )
    slip_modes = modes.reshape(2, devices, 8, edge).transpose(0, 2, 1, 3).reshape(2, 8, devices * edge)
    return (*out, slip_modes)


def solution(mesh):
    return jax.shard_map(
        body,
        mesh=mesh,
        in_specs=(
            P("strike", "depth"),
            P("strike", "depth"),
            P("strike", "depth"),
            P("strike", "depth"),
            P("strike", "depth"),
            P("strike", "depth"),
            P(None, ("strike", "depth"), None),
            P(None, None, ("strike", "depth"), None),
        ),
        out_specs=(P("strike", "depth"), P("strike", "depth"), P(None, ("strike", "depth"), None)),
        check_vma=False,
    )
```

```python
import functools
import math

import jax
import jax.numpy as jnp
import ml_dtypes
import numpy as np
from jax import lax
from jax.experimental import pallas as pl
from jax.experimental.pallas import tpu as pltpu
from jax.sharding import PartitionSpec as P

NEWTON_ITERS = 4
DAMPING = 0.5
RELAXATION = 0.5
ADVANCE = 0.5
LAGS = 8
FORWARD = ((0, 384), (384, 128))
INVERSE = ((0, 256), (256, 256))
SLOTS = (((0, 1, 2, 3),), ((0, 1), (2,), (3,)))
PAIR = 2
GRANT = 16 << 20
WIDE = 24 << 20
ALL = ("strike", "depth")
F32 = jnp.float32
BF16 = jnp.bfloat16
NN = (((1,), (0,)), ((), ()))
NT = (((1,), (1,)), ((), ()))
TN = (((0,), (0,)), ((), ()))
VMEM = pl.BlockSpec(memory_space=pltpu.VMEM)
SMEM = pl.BlockSpec(memory_space=pltpu.SMEM)
HBM = pl.BlockSpec(memory_space=pltpu.HBM)


def split_np(table):
    high = table.astype(ml_dtypes.bfloat16)
    low = (table - high.astype(np.float64)).astype(ml_dtypes.bfloat16)
    return high, low


def split(value):
    high = value.astype(BF16)
    return high, (value - high.astype(F32)).astype(BF16)


def in_hbm(*values):
    return [pltpu.with_memory_space_constraint(jnp.asarray(v), pltpu.HBM) for v in values]


def dot3(left, right, dims):
    (left_axis,), (right_axis,) = dims[0]
    return lax.dot_general(
        jnp.concatenate([left[0], left[0], left[1]], axis=left_axis),
        jnp.concatenate([right[0], right[1], right[0]], axis=right_axis),
        dims,
        preferred_element_type=F32,
    )


def depth_seeds(depth_len, blocks):
    cells = depth_len // 4
    cell = np.arange(cells)
    turn = 2.0 * np.pi / depth_len
    coarse = turn * ((8 * np.arange(blocks)[:, None] * cell[None]) % depth_len)
    fine = turn * ((np.arange(8)[:, None] * cell[None]) % depth_len)
    pack = lambda angle: np.stack([np.cos(angle), np.sin(angle)]).astype(np.float32)
    return pack(coarse), pack(fine)


def table_kernel(coarse_ref, fine_ref, high_ref, low_ref):
    blocks = coarse_ref.shape[1]
    cos_a, sin_a = coarse_ref[0], coarse_ref[1]
    for cls in range(4):
        for half in range(2):
            row = 4 * half + cls
            cos_b, sin_b = fine_ref[0, row : row + 1, :], fine_ref[1, row : row + 1, :]
            for part, value in enumerate(
                (cos_a * cos_b - sin_a * sin_b, sin_a * cos_b + cos_a * sin_b)
            ):
                high, low = split(value)
                rows = pl.ds((part * 2 + half) * blocks, blocks)
                high_ref[cls, rows, :] = high
                low_ref[cls, rows, :] = low


def depth_tables(depth_len, blocks):
    coarse, fine = depth_seeds(depth_len, blocks)
    shape = jax.ShapeDtypeStruct((4, 4 * blocks, depth_len // 4), BF16)
    return pl.pallas_call(
        table_kernel,
        out_shape=(shape, shape),
        in_specs=[VMEM, VMEM],
        out_specs=(VMEM, VMEM),
        compiler_params=pltpu.CompilerParams(vmem_limit_bytes=GRANT),
        name="depth_tables",
        cost_estimate=pl.CostEstimate(flops=10_000_000, bytes_accessed=5_000_000, transcendentals=0),
    )(coarse, fine)


def depth_forward_kernel(first, column, me_ref, own_ref, one_ref, two_ref, three_ref, high_ref, low_ref, *refs):
    rows, cells = own_ref.shape
    blocks = high_ref.shape[1] // 4
    cols = pl.ds(column, cells)
    me = me_ref[0]
    swap = (me & 1) == 1
    tau = (1 - 2 * (me & 1)).astype(F32)
    sigma = (1 - (me & 2)).astype(F32)
    even, odd = own_ref[...] + two_ref[...], one_ref[...] + three_ref[...]
    left, right = sigma * (own_ref[...] - two_ref[...]), sigma * (one_ref[...] - three_ref[...])
    both = jnp.concatenate(
        [jnp.where(swap, right, left), jnp.where(swap, left, right)], axis=0
    )

    def put(cls, real, imag):
        for plane, value in enumerate((real, imag)):
            for half in range(2):
                part = value[half * blocks : (half + 1) * blocks]
                slot = cls * 4 + plane * 2 + half
                if first:
                    refs[0][slot] = part
                else:
                    start = plane * 8 + half * 4 + cls
                    refs[1][pl.ds(start, blocks, stride=16), :] = part + refs[0][slot]

    def turn(cls, parts):
        return dot3((high_ref[cls, :, cols], low_ref[cls, :, cols]), parts, NT)

    top = 2 * blocks
    for cls, value in ((0, even + odd), (2, tau * (even - odd))):
        res = turn(cls, split(value))
        put(cls, res[:top], -res[top:])
    parts = split(both)
    res = turn(1, parts)
    put(1, res[:top, :rows] - res[top:, rows:], -(res[top:, :rows] + res[:top, rows:]))
    res = turn(3, parts)
    put(3, res[:top, :rows] + res[top:, rows:], res[:top, rows:] - res[top:, :rows])


def depth_forward(column, me, parts, tables, held=None):
    blocks = tables[0].shape[1] // 4
    rows = parts[0].shape[0]
    first = held is None
    shape = (16, blocks, rows) if first else (blocks * 16, rows)
    return pl.pallas_call(
        functools.partial(depth_forward_kernel, first, column),
        out_shape=jax.ShapeDtypeStruct(shape, F32),
        in_specs=[SMEM] + [VMEM] * (6 if first else 7),
        out_specs=VMEM,
        compiler_params=pltpu.CompilerParams(vmem_limit_bytes=GRANT),
        name="depth_forward",
        cost_estimate=pl.CostEstimate(flops=1_200_000_000, bytes_accessed=4_000_000, transcendentals=0),
    )(me, *parts, *tables, *(() if first else (held,)))


def depth_inverse_kernel(column, me_ref, y_ref, high_ref, low_ref, own_ref, one_ref, two_ref, three_ref):
    rows, cells = own_ref.shape
    blocks = high_ref.shape[1] // 4
    cols = pl.ds(column, cells)
    me = me_ref[0]
    swap = (me & 1) == 1
    tau = (1 - 2 * (me & 1)).astype(F32)
    sigma = (1 - (me & 2)).astype(F32)

    def get(cls, plane):
        value = jnp.concatenate(
            [y_ref[pl.ds(plane * 8 + half * 4 + cls, blocks, stride=16), :] for half in range(2)],
            axis=0,
        )
        if cls == 0:
            first = lax.broadcasted_iota(jnp.int32, value.shape, 0) == 0
            value = jnp.where(first, 0.5 * value, value)
        return split(value.T)

    def turn(cls, *lines):
        left = [
            jnp.concatenate([jnp.concatenate(line, axis=1) for line in part], axis=0)
            for part in zip(*[[(a, b) for a, b in zip(*line)] for line in lines])
        ]
        return dot3(left, (high_ref[cls, :, cols], low_ref[cls, :, cols]), NN)

    def minus(parts):
        return [-part for part in parts]

    real, imag = get(0, 0), get(0, 1)
    zero = turn(0, (real, minus(imag)))
    real, imag = get(2, 0), get(2, 1)
    two = tau * turn(2, (real, minus(imag)))
    real, imag = get(1, 0), get(1, 1)
    odd = turn(1, (real, minus(imag)), (minus(imag), minus(real)))
    real, imag = get(3, 0), get(3, 1)
    odd = sigma * (odd + turn(3, (real, minus(imag)), (imag, real)))
    low, high = odd[:rows], odd[rows:]
    base, turned = zero + two, jnp.where(swap, high, low)
    own_ref[...] = base + turned
    two_ref[...] = base - turned
    base, turned = zero - two, jnp.where(swap, low, high)
    one_ref[...] = base + turned
    three_ref[...] = base - turned


def depth_inverse(column, width, me, waves, tables):
    rows = waves.shape[1]
    shape = jax.ShapeDtypeStruct((rows, width), F32)
    return pl.pallas_call(
        functools.partial(depth_inverse_kernel, column),
        out_shape=(shape,) * 4,
        in_specs=[SMEM] + [VMEM] * 3,
        out_specs=(VMEM,) * 4,
        compiler_params=pltpu.CompilerParams(vmem_limit_bytes=GRANT),
        name="depth_inverse",
        cost_estimate=pl.CostEstimate(flops=1_200_000_000, bytes_accessed=4_000_000, transcendentals=0),
    )(me, waves, *tables)


def strike_tables(edge, scale):
    turn = 2.0 * np.pi / edge
    angle = turn * (np.outer(np.arange(edge), np.arange(edge)) % edge)
    waves = np.stack([*split_np(np.cos(angle)), *split_np(np.sin(angle))])
    twist = 2.0 * np.pi / (edge * edge) * np.outer(np.arange(edge), np.arange(edge))
    twist = np.stack([np.cos(twist), np.sin(twist)]) * scale
    return waves, np.concatenate([twist, 2.0 * twist]).astype(np.float32)


def strike_kernel(
    x_ref, gain_hbm, past_hbm, wave_ref, twist_ref, modes_hbm, out_ref,
    gain_ref, past_ref, held_ref, modes_ref, sems,
):
    edge = twist_ref.shape[1]
    pairs = ((gain_hbm, gain_ref), (past_hbm, past_ref))
    loads = [pltpu.make_async_copy(a, b, sems.at[n]) for n, (a, b) in enumerate(pairs)]
    for load in loads:
        load.start()

    def lines(group):
        return range(group * PAIR, (group + 1) * PAIR)

    def lanes(value, place):
        part = value[:, place * edge : (place + 1) * edge]
        return part[:edge], part[edge:]

    def gather(m):
        return jnp.concatenate(
            [x_ref[pl.ds(plane * 8 + m, edge, stride=16), :] for plane in range(2)], axis=0
        )

    def block(sign, part):
        cosine, sine = wave_ref[part], wave_ref[2 + part]
        left, right = (sine, -sine) if sign > 0 else (-sine, sine)
        return jnp.concatenate(
            [jnp.concatenate([cosine, left], axis=1), jnp.concatenate([right, cosine], axis=1)], axis=0
        )

    def rotate(value, sign, cosine, sine):
        rows = []
        for place in range(PAIR):
            real, imag = lanes(value, place)
            if sign > 0:
                rows.append([real * cosine + imag * sine, imag * cosine - real * sine])
            else:
                rows.append([real * cosine - imag * sine, imag * cosine + real * sine])
        return jnp.concatenate([jnp.concatenate(row, axis=1) for row in rows], axis=0)

    forward = (block(1, 0), block(1, 1))
    for group in range(8 // PAIR):
        value = jnp.concatenate([gather(m) for m in lines(group)], axis=1)
        value = dot3(forward, split(value), NN)
        value = dot3(forward, split(rotate(value, 1, twist_ref[0], twist_ref[1])), NT)
        for place, m in enumerate(lines(group)):
            for plane, part in enumerate(lanes(value, place)):
                held_ref[plane, m] = part
                modes_ref[plane, pl.ds(m, edge, stride=8), :] = part
    save = pltpu.make_async_copy(modes_ref, modes_hbm, sems.at[2])
    save.start()
    for load in loads:
        load.wait()
    backward = (block(-1, 0), block(-1, 1))
    for group in range(8 // PAIR):
        value = jnp.concatenate(
            [
                jnp.concatenate(
                    [gain_ref[m] * held_ref[plane, m] + past_ref[plane, m] for plane in range(2)], axis=0
                )
                for m in lines(group)
            ],
            axis=1,
        )
        value = dot3(backward, split(value), NN)
        value = dot3(backward, split(rotate(value, -1, twist_ref[2], twist_ref[3])), NT)
        for place, m in enumerate(lines(group)):
            for plane, part in enumerate(lanes(value, place)):
                out_ref[pl.ds(plane * 8 + m, edge, stride=16), :] = part
    save.wait()


def strike_both(pencil, gain, past, tables):
    waves, twist = tables
    edge = twist.shape[1]
    modes = (2, edge * 8, edge)
    return pl.pallas_call(
        strike_kernel,
        out_shape=(
            pltpu.HBM(modes, F32),
            jax.ShapeDtypeStruct((edge * 16, edge), F32),
        ),
        in_specs=[VMEM, HBM, HBM, VMEM, VMEM],
        out_specs=(HBM, VMEM),
        scratch_shapes=[
            pltpu.VMEM(gain.shape, F32),
            pltpu.VMEM(past.shape, F32),
            pltpu.VMEM(past.shape, F32),
            pltpu.VMEM(modes, F32),
            pltpu.SemaphoreType.DMA((3,)),
        ],
        compiler_params=pltpu.CompilerParams(vmem_limit_bytes=WIDE),
        name="strike_both",
        cost_estimate=pl.CostEstimate(flops=1_600_000_000, bytes_accessed=6_000_000, transcendentals=0),
    )(pencil, *in_hbm(gain, past), waves, twist)


def past_kernel(kernel_ref, history_ref, gain_ref, past_ref):
    for tile in range(kernel_ref.shape[2] // 128):
        cols = pl.ds(tile * 128, 128)
        gain_ref[:, tile, :] = kernel_ref[0, :, cols]
        for plane in range(2):
            total = kernel_ref[1, :, cols] * history_ref[0, plane, :, cols]
            for lag in range(1, LAGS):
                total = total + kernel_ref[lag + 1, :, cols] * history_ref[lag, plane, :, cols]
            past_ref[plane, :, tile, :] = total


def past_sum(kernel, history):
    length = kernel.shape[2]
    block = 2048
    return pl.pallas_call(
        past_kernel,
        grid=(length // block,),
        out_shape=(
            pltpu.HBM((8, length // 128, 128), F32),
            pltpu.HBM((2, 8, length // 128, 128), F32),
        ),
        in_specs=[
            pl.BlockSpec((LAGS + 1, 8, block), lambda i: (0, 0, i)),
            pl.BlockSpec((LAGS, 2, 8, block), lambda i: (0, 0, 0, i)),
        ],
        out_specs=(
            pl.BlockSpec((8, block // 128, 128), lambda i: (0, i, 0)),
            pl.BlockSpec((2, 8, block // 128, 128), lambda i: (0, 0, i, 0)),
        ),
        compiler_params=pltpu.CompilerParams(vmem_limit_bytes=WIDE),
        name="past_sum",
        cost_estimate=pl.CostEstimate(flops=4_200_000, bytes_accessed=14_700_000, transcendentals=0),
    )(*in_hbm(kernel, history))


def newton_parts(rate, scaling, strength):
    scaled = rate * scaling
    magnitude = jnp.abs(scaled)
    square = 1.0 + scaled * scaled
    inverse = lax.rsqrt(square)
    positive = jnp.log(magnitude + square * inverse)
    friction = strength * jnp.where(scaled < 0, -positive, positive)
    return friction, 1.0 + (strength * scaling) * (inverse * (1.0 / DAMPING))


STEP = RELAXATION / DAMPING


def start_kernel(rate_ref, state_ref, weak_ref, strength_ref, stress_ref, scale_ref, rest_ref, gain_ref):
    scaling = 0.5 * jnp.exp(weak_ref[...] * state_ref[...])
    rate = rate_ref[...]
    friction, divisor = newton_parts(rate, scaling, strength_ref[...])
    gain = STEP / divisor
    scale_ref[...] = scaling
    gain_ref[...] = gain
    rest_ref[...] = rate + gain * (stress_ref[...] - DAMPING * rate - friction)


def friction_start(rate_prev, log_state, weakening, strength, pre_stress):
    rows, cells = rate_prev.shape
    spec = pl.BlockSpec((64, cells), lambda i: (i, 0))
    shape = jax.ShapeDtypeStruct((rows, cells), F32)
    return pl.pallas_call(
        start_kernel,
        grid=(rows // 64,),
        out_shape=(shape,) * 3,
        in_specs=[spec] * 5,
        out_specs=(spec,) * 3,
        compiler_params=pltpu.CompilerParams(vmem_limit_bytes=GRANT),
        name="friction_start",
        cost_estimate=pl.CostEstimate(flops=20_000_000, bytes_accessed=8_000_000, transcendentals=1_000_000),
    )(rate_prev, log_state, weakening, strength, pre_stress)


def friction_kernel(
    slots, column, me_ref, scale_ref, rest_ref, gain_ref, strength_ref, stress_ref, slip_ref, *refs
):
    velocity_hbm, new_hbm, velocity_ref, new_ref, sems = refs[-5:]
    parts = refs[: len(slots)]
    edge, width = parts[0].shape
    cols = pl.ds(column, width)
    saves = []
    for place, (slot, ref) in enumerate(zip(slots, parts)):
        rows = pl.ds(pl.multiple_of((me_ref[0] ^ slot) * edge, edge), edge)
        elastic = ref[...]
        scaling, strength = scale_ref[rows, cols], strength_ref[rows, cols]
        total = stress_ref[rows, cols] + elastic
        rate = rest_ref[rows, cols] + gain_ref[rows, cols] * elastic
        for sweep in range(NEWTON_ITERS - 1):
            friction, divisor = newton_parts(rate, scaling, strength)
            rate = rate + STEP * (total - DAMPING * rate - friction) / divisor
        velocity_ref[place] = rate
        new_ref[place] = slip_ref[rows, cols] + ADVANCE * rate
        for n, (source, target) in enumerate(((velocity_ref, velocity_hbm), (new_ref, new_hbm))):
            save = pltpu.make_async_copy(source.at[place], target.at[rows, cols], sems.at[place, n])
            save.start()
            saves.append(save)
    for save in saves:
        save.wait()


def friction_finish(slots, column, me, elastic, start, strength, pre_stress, fault_slip, held=()):
    edge, width = elastic[0].shape
    shape = jax.ShapeDtypeStruct(fault_slip.shape, F32)
    count = 7 + len(slots)
    return pl.pallas_call(
        functools.partial(friction_kernel, slots, column),
        in_specs=[SMEM] + [VMEM] * (6 + len(slots)) + [HBM] * len(held),
        out_specs=(HBM, HBM),
        out_shape=(shape, shape),
        scratch_shapes=[
            pltpu.VMEM((len(slots), edge, width), F32),
            pltpu.VMEM((len(slots), edge, width), F32),
            pltpu.SemaphoreType.DMA((len(slots), 2)),
        ],
        input_output_aliases={count + n: n for n in range(len(held))},
        compiler_params=pltpu.CompilerParams(vmem_limit_bytes=GRANT),
        name="friction_finish",
        cost_estimate=pl.CostEstimate(flops=20_000_000, bytes_accessed=5_000_000, transcendentals=1_000_000),
    )(me, *start, strength, pre_stress, fault_slip, *elastic, *in_hbm(*held))


def exchange(parts, size):
    swap = lambda part, k: lax.ppermute(part, "depth", [(place, place ^ k) for place in range(size)])
    moved = {k: swap(parts[k], k) for k in (2, 3, 1)}
    return [parts[0]] + [moved[k] for k in (1, 2, 3)]


def body(fault_slip, rate_prev, log_state, weakening, strength, pre_stress, kernel, history):
    rows, cells = fault_slip.shape
    depth_size = lax.axis_size("depth")
    devices = lax.axis_size("strike") * depth_size
    edge = rows // depth_size
    depth_len = cells * depth_size
    place = lax.axis_index("depth")
    me = place.reshape(1)
    block = lambda source, k, part: lax.dynamic_slice(
        source, ((place ^ k) * edge, part[0]), (edge, part[1])
    )
    far = [block(fault_slip, k, FORWARD[0]) for k in (2, 3)]
    source, *far = lax.optimization_barrier((fault_slip, *far))
    near = [block(source, k, FORWARD[0]) for k in (0, 1)]
    lines = [exchange(near + far, depth_size)]
    for part in FORWARD[1:]:
        lines.append(exchange([block(source, k, part) for k in range(depth_size)], depth_size))
    tables = depth_tables(depth_len, devices)
    gain, past = past_sum(kernel, history)
    waves = None
    for (column, _), parts in zip(FORWARD, lines):
        waves = depth_forward(column, me, parts, tables, waves)
    pencil = lax.all_to_all(waves.reshape(devices, 16, edge), ALL, 0, 0)
    scale = 1.0 / math.sqrt(depth_len * edge * devices)
    modes, waves = strike_both(
        pencil.reshape(devices * 16, edge), gain, past, strike_tables(edge, scale)
    )
    start = friction_start(rate_prev, log_state, weakening, strength, pre_stress)
    waves = lax.all_to_all(waves.reshape(devices, 16, edge), ALL, 0, 0).reshape(devices * 16, edge)
    elastic = [
        exchange(depth_inverse(column, width, me, waves, tables), depth_size)
        for column, width in INVERSE
    ]
    out = ()
    for (column, _), parts, groups in zip(INVERSE, elastic, SLOTS):
        for slots in groups:
            parts_now = [parts[slot] for slot in slots]
            out = friction_finish(
                slots, column, me, parts_now, start, strength, pre_stress, fault_slip, out
            )
    slip_modes = modes.reshape(2, devices, 8, edge).transpose(0, 2, 1, 3).reshape(2, 8, devices * edge)
    return (*out, slip_modes)


def solution(mesh):
    return jax.shard_map(
        body,
        mesh=mesh,
        in_specs=(
            P("strike", "depth"),
            P("strike", "depth"),
            P("strike", "depth"),
            P("strike", "depth"),
            P("strike", "depth"),
            P("strike", "depth"),
            P(None, ("strike", "depth"), None),
            P(None, None, ("strike", "depth"), None),
        ),
        out_specs=(P("strike", "depth"), P("strike", "depth"), P(None, ("strike", "depth"), None)),
        check_vma=False,
    )
```

```python
import functools
import math

import jax
import jax.numpy as jnp
import ml_dtypes
import numpy as np
from jax import lax
from jax.experimental import pallas as pl
from jax.experimental.pallas import tpu as pltpu
from jax.sharding import PartitionSpec as P

NEWTON_ITERS = 4
DAMPING = 0.5
RELAXATION = 0.5
ADVANCE = 0.5
LAGS = 8
FORWARD = ((0, 384), (384, 128))
INVERSE = ((0, 256), (256, 256))
SLOTS = (((0, 1, 2, 3),), ((0, 1), (2,), (3,)))
PAIR = 2
GRANT = 16 << 20
WIDE = 24 << 20
ALL = ("strike", "depth")
F32 = jnp.float32
BF16 = jnp.bfloat16
NN = (((1,), (0,)), ((), ()))
NT = (((1,), (1,)), ((), ()))
TN = (((0,), (0,)), ((), ()))
VMEM = pl.BlockSpec(memory_space=pltpu.VMEM)
SMEM = pl.BlockSpec(memory_space=pltpu.SMEM)
HBM = pl.BlockSpec(memory_space=pltpu.HBM)


def split_np(table):
    high = table.astype(ml_dtypes.bfloat16)
    low = (table - high.astype(np.float64)).astype(ml_dtypes.bfloat16)
    return high, low


def split(value):
    high = value.astype(BF16)
    return high, (value - high.astype(F32)).astype(BF16)


def in_hbm(*values):
    return [pltpu.with_memory_space_constraint(jnp.asarray(v), pltpu.HBM) for v in values]


def dot3(left, right, dims):
    (left_axis,), (right_axis,) = dims[0]
    return lax.dot_general(
        jnp.concatenate([left[0], left[0], left[1]], axis=left_axis),
        jnp.concatenate([right[0], right[1], right[0]], axis=right_axis),
        dims,
        preferred_element_type=F32,
    )


def depth_seeds(depth_len, blocks):
    cells = depth_len // 4
    cell = np.arange(cells)
    turn = 2.0 * np.pi / depth_len
    coarse = turn * ((8 * np.arange(blocks)[:, None] * cell[None]) % depth_len)
    fine = turn * ((np.arange(8)[:, None] * cell[None]) % depth_len)
    pack = lambda angle: np.stack([np.cos(angle), np.sin(angle)]).astype(np.float32)
    return pack(coarse), pack(fine)


def table_kernel(coarse_ref, fine_ref, high_ref, low_ref):
    blocks = coarse_ref.shape[1]
    cos_a, sin_a = coarse_ref[0], coarse_ref[1]
    for cls in range(4):
        for half in range(2):
            row = 4 * half + cls
            cos_b, sin_b = fine_ref[0, row : row + 1, :], fine_ref[1, row : row + 1, :]
            for part, value in enumerate(
                (cos_a * cos_b - sin_a * sin_b, sin_a * cos_b + cos_a * sin_b)
            ):
                high, low = split(value)
                rows = pl.ds((part * 2 + half) * blocks, blocks)
                high_ref[cls, rows, :] = high
                low_ref[cls, rows, :] = low


def depth_tables(depth_len, blocks):
    coarse, fine = depth_seeds(depth_len, blocks)
    shape = jax.ShapeDtypeStruct((4, 4 * blocks, depth_len // 4), BF16)
    return pl.pallas_call(
        table_kernel,
        out_shape=(shape, shape),
        in_specs=[VMEM, VMEM],
        out_specs=(VMEM, VMEM),
        compiler_params=pltpu.CompilerParams(vmem_limit_bytes=GRANT),
        name="depth_tables",
        cost_estimate=pl.CostEstimate(flops=10_000_000, bytes_accessed=5_000_000, transcendentals=0),
    )(coarse, fine)


def depth_forward_kernel(first, column, me_ref, own_ref, one_ref, two_ref, three_ref, high_ref, low_ref, *refs):
    rows, cells = own_ref.shape
    blocks = high_ref.shape[1] // 4
    cols = pl.ds(column, cells)
    me = me_ref[0]
    swap = (me & 1) == 1
    tau = (1 - 2 * (me & 1)).astype(F32)
    sigma = (1 - (me & 2)).astype(F32)
    even, odd = own_ref[...] + two_ref[...], one_ref[...] + three_ref[...]
    left, right = sigma * (own_ref[...] - two_ref[...]), sigma * (one_ref[...] - three_ref[...])
    both = jnp.concatenate(
        [jnp.where(swap, right, left), jnp.where(swap, left, right)], axis=0
    )

    def put(cls, real, imag):
        for plane, value in enumerate((real, imag)):
            for half in range(2):
                part = value[half * blocks : (half + 1) * blocks]
                slot = cls * 4 + plane * 2 + half
                if first:
                    refs[0][slot] = part
                else:
                    start = plane * 8 + half * 4 + cls
                    refs[1][pl.ds(start, blocks, stride=16), :] = part + refs[0][slot]

    def turn(cls, parts):
        return dot3((high_ref[cls, :, cols], low_ref[cls, :, cols]), parts, NT)

    top = 2 * blocks
    for cls, value in ((0, even + odd), (2, tau * (even - odd))):
        res = turn(cls, split(value))
        put(cls, res[:top], -res[top:])
    parts = split(both)
    res = turn(1, parts)
    put(1, res[:top, :rows] - res[top:, rows:], -(res[top:, :rows] + res[:top, rows:]))
    res = turn(3, parts)
    put(3, res[:top, :rows] + res[top:, rows:], res[:top, rows:] - res[top:, :rows])


def depth_forward(column, me, parts, tables, held=None):
    blocks = tables[0].shape[1] // 4
    rows = parts[0].shape[0]
    first = held is None
    shape = (16, blocks, rows) if first else (blocks * 16, rows)
    return pl.pallas_call(
        functools.partial(depth_forward_kernel, first, column),
        out_shape=jax.ShapeDtypeStruct(shape, F32),
        in_specs=[SMEM] + [VMEM] * (6 if first else 7),
        out_specs=VMEM,
        compiler_params=pltpu.CompilerParams(vmem_limit_bytes=GRANT),
        name="depth_forward",
        cost_estimate=pl.CostEstimate(flops=1_200_000_000, bytes_accessed=4_000_000, transcendentals=0),
    )(me, *parts, *tables, *(() if first else (held,)))


def depth_inverse_kernel(column, me_ref, y_ref, high_ref, low_ref, own_ref, one_ref, two_ref, three_ref):
    rows, cells = own_ref.shape
    blocks = high_ref.shape[1] // 4
    cols = pl.ds(column, cells)
    me = me_ref[0]
    swap = (me & 1) == 1
    tau = (1 - 2 * (me & 1)).astype(F32)
    sigma = (1 - (me & 2)).astype(F32)

    def get(cls, plane):
        value = jnp.concatenate(
            [y_ref[pl.ds(plane * 8 + half * 4 + cls, blocks, stride=16), :] for half in range(2)],
            axis=0,
        )
        if cls == 0:
            first = lax.broadcasted_iota(jnp.int32, value.shape, 0) == 0
            value = jnp.where(first, 0.5 * value, value)
        return split(value.T)

    def turn(cls, *lines):
        left = [
            jnp.concatenate([jnp.concatenate(line, axis=1) for line in part], axis=0)
            for part in zip(*[[(a, b) for a, b in zip(*line)] for line in lines])
        ]
        return dot3(left, (high_ref[cls, :, cols], low_ref[cls, :, cols]), NN)

    def minus(parts):
        return [-part for part in parts]

    real, imag = get(0, 0), get(0, 1)
    zero = turn(0, (real, minus(imag)))
    real, imag = get(2, 0), get(2, 1)
    two = tau * turn(2, (real, minus(imag)))
    real, imag = get(1, 0), get(1, 1)
    odd = turn(1, (real, minus(imag)), (minus(imag), minus(real)))
    real, imag = get(3, 0), get(3, 1)
    odd = sigma * (odd + turn(3, (real, minus(imag)), (imag, real)))
    low, high = odd[:rows], odd[rows:]
    base, turned = zero + two, jnp.where(swap, high, low)
    own_ref[...] = base + turned
    two_ref[...] = base - turned
    base, turned = zero - two, jnp.where(swap, low, high)
    one_ref[...] = base + turned
    three_ref[...] = base - turned


def depth_inverse(column, width, me, waves, tables):
    rows = waves.shape[1]
    shape = jax.ShapeDtypeStruct((rows, width), F32)
    return pl.pallas_call(
        functools.partial(depth_inverse_kernel, column),
        out_shape=(shape,) * 4,
        in_specs=[SMEM] + [VMEM] * 3,
        out_specs=(VMEM,) * 4,
        compiler_params=pltpu.CompilerParams(vmem_limit_bytes=GRANT),
        name="depth_inverse",
        cost_estimate=pl.CostEstimate(flops=1_200_000_000, bytes_accessed=4_000_000, transcendentals=0),
    )(me, waves, *tables)


def strike_tables(edge, scale):
    turn = 2.0 * np.pi / edge
    angle = turn * (np.outer(np.arange(edge), np.arange(edge)) % edge)
    waves = np.stack([*split_np(np.cos(angle)), *split_np(np.sin(angle))])
    twist = 2.0 * np.pi / (edge * edge) * np.outer(np.arange(edge), np.arange(edge))
    twist = np.stack([np.cos(twist), np.sin(twist)]) * scale
    return waves, np.concatenate([twist, 2.0 * twist]).astype(np.float32)


def strike_kernel(
    x_ref, gain_hbm, past_hbm, wave_ref, twist_ref, modes_hbm, out_ref,
    gain_ref, past_ref, held_ref, modes_ref, sems,
):
    edge = twist_ref.shape[1]
    pairs = ((gain_hbm, gain_ref), (past_hbm, past_ref))
    loads = [pltpu.make_async_copy(a, b, sems.at[n]) for n, (a, b) in enumerate(pairs)]
    for load in loads:
        load.start()

    def lines(group):
        return range(group * PAIR, (group + 1) * PAIR)

    def lanes(value, place):
        part = value[:, place * edge : (place + 1) * edge]
        return part[:edge], part[edge:]

    def gather(m):
        return jnp.concatenate(
            [x_ref[pl.ds(plane * 8 + m, edge, stride=16), :] for plane in range(2)], axis=0
        )

    def block(sign, part):
        cosine, sine = wave_ref[part], wave_ref[2 + part]
        left, right = (sine, -sine) if sign > 0 else (-sine, sine)
        return jnp.concatenate(
            [jnp.concatenate([cosine, left], axis=1), jnp.concatenate([right, cosine], axis=1)], axis=0
        )

    def rotate(value, sign, cosine, sine):
        rows = []
        for place in range(PAIR):
            real, imag = lanes(value, place)
            if sign > 0:
                rows.append([real * cosine + imag * sine, imag * cosine - real * sine])
            else:
                rows.append([real * cosine - imag * sine, imag * cosine + real * sine])
        return jnp.concatenate([jnp.concatenate(row, axis=1) for row in rows], axis=0)

    groups = 8 // PAIR
    forward = (block(1, 0), block(1, 1))
    kept = None
    for group in range(groups + 1):
        before, kept = kept, None
        if group < groups:
            value = jnp.concatenate([gather(m) for m in lines(group)], axis=1)
            kept = dot3(forward, split(value), NN)
        if group > 0:
            value = dot3(forward, split(rotate(before, 1, twist_ref[0], twist_ref[1])), NT)
            for place, m in enumerate(lines(group - 1)):
                for plane, part in enumerate(lanes(value, place)):
                    held_ref[plane, m] = part
                    modes_ref[plane, pl.ds(m, edge, stride=8), :] = part
    save = pltpu.make_async_copy(modes_ref, modes_hbm, sems.at[2])
    save.start()
    for load in loads:
        load.wait()
    backward = (block(-1, 0), block(-1, 1))
    for group in range(groups + 1):
        before, kept = kept, None
        if group < groups:
            value = jnp.concatenate(
                [
                    jnp.concatenate(
                        [
                            gain_ref[m] * held_ref[plane, m] + past_ref[plane, m]
                            for plane in range(2)
                        ],
                        axis=0,
                    )
                    for m in lines(group)
                ],
                axis=1,
            )
            kept = dot3(backward, split(value), NN)
        if group > 0:
            value = dot3(backward, split(rotate(before, -1, twist_ref[2], twist_ref[3])), NT)
            for place, m in enumerate(lines(group - 1)):
                for plane, part in enumerate(lanes(value, place)):
                    out_ref[pl.ds(plane * 8 + m, edge, stride=16), :] = part
    save.wait()


def strike_both(pencil, gain, past, tables):
    waves, twist = tables
    edge = twist.shape[1]
    modes = (2, edge * 8, edge)
    return pl.pallas_call(
        strike_kernel,
        out_shape=(
            pltpu.HBM(modes, F32),
            jax.ShapeDtypeStruct((edge * 16, edge), F32),
        ),
        in_specs=[VMEM, HBM, HBM, VMEM, VMEM],
        out_specs=(HBM, VMEM),
        scratch_shapes=[
            pltpu.VMEM(gain.shape, F32),
            pltpu.VMEM(past.shape, F32),
            pltpu.VMEM(past.shape, F32),
            pltpu.VMEM(modes, F32),
            pltpu.SemaphoreType.DMA((3,)),
        ],
        compiler_params=pltpu.CompilerParams(vmem_limit_bytes=WIDE),
        name="strike_both",
        cost_estimate=pl.CostEstimate(flops=1_600_000_000, bytes_accessed=6_000_000, transcendentals=0),
    )(pencil, *in_hbm(gain, past), waves, twist)


def past_kernel(kernel_ref, history_ref, gain_ref, past_ref):
    for tile in range(kernel_ref.shape[2] // 128):
        cols = pl.ds(tile * 128, 128)
        gain_ref[:, tile, :] = kernel_ref[0, :, cols]
        for plane in range(2):
            total = kernel_ref[1, :, cols] * history_ref[0, plane, :, cols]
            for lag in range(1, LAGS):
                total = total + kernel_ref[lag + 1, :, cols] * history_ref[lag, plane, :, cols]
            past_ref[plane, :, tile, :] = total


def past_sum(kernel, history):
    length = kernel.shape[2]
    block = 2048
    return pl.pallas_call(
        past_kernel,
        grid=(length // block,),
        out_shape=(
            pltpu.HBM((8, length // 128, 128), F32),
            pltpu.HBM((2, 8, length // 128, 128), F32),
        ),
        in_specs=[
            pl.BlockSpec((LAGS + 1, 8, block), lambda i: (0, 0, i)),
            pl.BlockSpec((LAGS, 2, 8, block), lambda i: (0, 0, 0, i)),
        ],
        out_specs=(
            pl.BlockSpec((8, block // 128, 128), lambda i: (0, i, 0)),
            pl.BlockSpec((2, 8, block // 128, 128), lambda i: (0, 0, i, 0)),
        ),
        compiler_params=pltpu.CompilerParams(vmem_limit_bytes=WIDE),
        name="past_sum",
        cost_estimate=pl.CostEstimate(flops=4_200_000, bytes_accessed=14_700_000, transcendentals=0),
    )(*in_hbm(kernel, history))


def newton_parts(rate, scaling, strength):
    scaled = rate * scaling
    magnitude = jnp.abs(scaled)
    square = 1.0 + scaled * scaled
    inverse = lax.rsqrt(square)
    positive = jnp.log(magnitude + square * inverse)
    friction = strength * jnp.where(scaled < 0, -positive, positive)
    return friction, 1.0 + (strength * scaling) * (inverse * (1.0 / DAMPING))


STEP = RELAXATION / DAMPING


def start_kernel(rate_ref, state_ref, weak_ref, strength_ref, stress_ref, scale_ref, rest_ref, gain_ref):
    scaling = 0.5 * jnp.exp(weak_ref[...] * state_ref[...])
    rate = rate_ref[...]
    friction, divisor = newton_parts(rate, scaling, strength_ref[...])
    gain = STEP / divisor
    scale_ref[...] = scaling
    gain_ref[...] = gain
    rest_ref[...] = rate + gain * (stress_ref[...] - DAMPING * rate - friction)


def friction_start(rate_prev, log_state, weakening, strength, pre_stress):
    rows, cells = rate_prev.shape
    spec = pl.BlockSpec((64, cells), lambda i: (i, 0))
    shape = jax.ShapeDtypeStruct((rows, cells), F32)
    return pl.pallas_call(
        start_kernel,
        grid=(rows // 64,),
        out_shape=(shape,) * 3,
        in_specs=[spec] * 5,
        out_specs=(spec,) * 3,
        compiler_params=pltpu.CompilerParams(vmem_limit_bytes=GRANT),
        name="friction_start",
        cost_estimate=pl.CostEstimate(flops=20_000_000, bytes_accessed=8_000_000, transcendentals=1_000_000),
    )(rate_prev, log_state, weakening, strength, pre_stress)


def friction_kernel(
    slots, column, me_ref, scale_ref, rest_ref, gain_ref, strength_ref, stress_ref, slip_ref, *refs
):
    velocity_hbm, new_hbm, velocity_ref, new_ref, sems = refs[-5:]
    parts = refs[: len(slots)]
    edge, width = parts[0].shape
    cols = pl.ds(column, width)
    saves = []
    for place, (slot, ref) in enumerate(zip(slots, parts)):
        rows = pl.ds(pl.multiple_of((me_ref[0] ^ slot) * edge, edge), edge)
        elastic = ref[...]
        scaling, strength = scale_ref[rows, cols], strength_ref[rows, cols]
        total = stress_ref[rows, cols] + elastic
        rate = rest_ref[rows, cols] + gain_ref[rows, cols] * elastic
        for sweep in range(NEWTON_ITERS - 1):
            friction, divisor = newton_parts(rate, scaling, strength)
            rate = rate + STEP * (total - DAMPING * rate - friction) / divisor
        velocity_ref[place] = rate
        new_ref[place] = slip_ref[rows, cols] + ADVANCE * rate
        for n, (source, target) in enumerate(((velocity_ref, velocity_hbm), (new_ref, new_hbm))):
            save = pltpu.make_async_copy(source.at[place], target.at[rows, cols], sems.at[place, n])
            save.start()
            saves.append(save)
    for save in saves:
        save.wait()


def friction_finish(slots, column, me, elastic, start, strength, pre_stress, fault_slip, held=()):
    edge, width = elastic[0].shape
    shape = jax.ShapeDtypeStruct(fault_slip.shape, F32)
    count = 7 + len(slots)
    return pl.pallas_call(
        functools.partial(friction_kernel, slots, column),
        in_specs=[SMEM] + [VMEM] * (6 + len(slots)) + [HBM] * len(held),
        out_specs=(HBM, HBM),
        out_shape=(shape, shape),
        scratch_shapes=[
            pltpu.VMEM((len(slots), edge, width), F32),
            pltpu.VMEM((len(slots), edge, width), F32),
            pltpu.SemaphoreType.DMA((len(slots), 2)),
        ],
        input_output_aliases={count + n: n for n in range(len(held))},
        compiler_params=pltpu.CompilerParams(vmem_limit_bytes=GRANT),
        name="friction_finish",
        cost_estimate=pl.CostEstimate(flops=20_000_000, bytes_accessed=5_000_000, transcendentals=1_000_000),
    )(me, *start, strength, pre_stress, fault_slip, *elastic, *in_hbm(*held))


def exchange(parts, size):
    swap = lambda part, k: lax.ppermute(part, "depth", [(place, place ^ k) for place in range(size)])
    moved = {k: swap(parts[k], k) for k in (2, 3, 1)}
    return [parts[0]] + [moved[k] for k in (1, 2, 3)]


def body(fault_slip, rate_prev, log_state, weakening, strength, pre_stress, kernel, history):
    rows, cells = fault_slip.shape
    depth_size = lax.axis_size("depth")
    devices = lax.axis_size("strike") * depth_size
    edge = rows // depth_size
    depth_len = cells * depth_size
    place = lax.axis_index("depth")
    me = place.reshape(1)
    block = lambda source, k, part: lax.dynamic_slice(
        source, ((place ^ k) * edge, part[0]), (edge, part[1])
    )
    far = [block(fault_slip, k, FORWARD[0]) for k in (2, 3)]
    source, *far = lax.optimization_barrier((fault_slip, *far))
    near = [block(source, k, FORWARD[0]) for k in (0, 1)]
    lines = [exchange(near + far, depth_size)]
    for part in FORWARD[1:]:
        lines.append(exchange([block(source, k, part) for k in range(depth_size)], depth_size))
    tables = depth_tables(depth_len, devices)
    gain, past = past_sum(kernel, history)
    waves = None
    for (column, _), parts in zip(FORWARD, lines):
        waves = depth_forward(column, me, parts, tables, waves)
    pencil = lax.all_to_all(waves.reshape(devices, 16, edge), ALL, 0, 0)
    scale = 1.0 / math.sqrt(depth_len * edge * devices)
    modes, waves = strike_both(
        pencil.reshape(devices * 16, edge), gain, past, strike_tables(edge, scale)
    )
    start = friction_start(rate_prev, log_state, weakening, strength, pre_stress)
    waves = lax.all_to_all(waves.reshape(devices, 16, edge), ALL, 0, 0).reshape(devices * 16, edge)
    elastic = [
        exchange(depth_inverse(column, width, me, waves, tables), depth_size)
        for column, width in INVERSE
    ]
    out = ()
    for (column, _), parts, groups in zip(INVERSE, elastic, SLOTS):
        for slots in groups:
            parts_now = [parts[slot] for slot in slots]
            out = friction_finish(
                slots, column, me, parts_now, start, strength, pre_stress, fault_slip, out
            )
    slip_modes = modes.reshape(2, devices, 8, edge).transpose(0, 2, 1, 3).reshape(2, 8, devices * edge)
    return (*out, slip_modes)


def solution(mesh):
    return jax.shard_map(
        body,
        mesh=mesh,
        in_specs=(
            P("strike", "depth"),
            P("strike", "depth"),
            P("strike", "depth"),
            P("strike", "depth"),
            P("strike", "depth"),
            P("strike", "depth"),
            P(None, ("strike", "depth"), None),
            P(None, None, ("strike", "depth"), None),
        ),
        out_specs=(P("strike", "depth"), P("strike", "depth"), P(None, ("strike", "depth"), None)),
        check_vma=False,
    )
```

```python
import functools
import math

import jax
import jax.numpy as jnp
import ml_dtypes
import numpy as np
from jax import lax
from jax.experimental import pallas as pl
from jax.experimental.pallas import tpu as pltpu
from jax.sharding import PartitionSpec as P

NEWTON_ITERS = 4
DAMPING = 0.5
RELAXATION = 0.5
ADVANCE = 0.5
LAGS = 8
FORWARD = ((0, 384), (384, 128))
INVERSE = ((0, 256), (256, 256))
SLOTS = (((0, 1, 2, 3),), ((0, 1), (2,), (3,)))
PAIR = 2
GRANT = 16 << 20
WIDE = 24 << 20
ALL = ("strike", "depth")
F32 = jnp.float32
BF16 = jnp.bfloat16
NN = (((1,), (0,)), ((), ()))
NT = (((1,), (1,)), ((), ()))
TN = (((0,), (0,)), ((), ()))
VMEM = pl.BlockSpec(memory_space=pltpu.VMEM)
SMEM = pl.BlockSpec(memory_space=pltpu.SMEM)
HBM = pl.BlockSpec(memory_space=pltpu.HBM)


def split_np(table):
    high = table.astype(ml_dtypes.bfloat16)
    low = (table - high.astype(np.float64)).astype(ml_dtypes.bfloat16)
    return high, low


def split(value):
    high = value.astype(BF16)
    return high, (value - high.astype(F32)).astype(BF16)


def in_hbm(*values):
    return [pltpu.with_memory_space_constraint(jnp.asarray(v), pltpu.HBM) for v in values]


def dot3(left, right, dims):
    (left_axis,), (right_axis,) = dims[0]
    return lax.dot_general(
        jnp.concatenate([left[0], left[0], left[1]], axis=left_axis),
        jnp.concatenate([right[0], right[1], right[0]], axis=right_axis),
        dims,
        preferred_element_type=F32,
    )


def place_of(mode, plane):
    half, cls = divmod(mode, 4)
    return (cls % 2) * 8 + plane * 4 + half * 2 + cls // 2


def depth_seeds(depth_len, blocks):
    cells = depth_len // 4
    cell = np.arange(cells)
    turn = 2.0 * np.pi / depth_len
    coarse = turn * ((8 * np.arange(blocks)[:, None] * cell[None]) % depth_len)
    fine = turn * ((np.arange(8)[:, None] * cell[None]) % depth_len)
    pack = lambda angle: np.stack([np.cos(angle), np.sin(angle)]).astype(np.float32)
    return pack(coarse), pack(fine)


def table_kernel(coarse_ref, fine_ref, high_ref, low_ref):
    blocks = coarse_ref.shape[1]
    cos_a, sin_a = coarse_ref[0], coarse_ref[1]
    for cls in range(4):
        for half in range(2):
            row = 4 * half + cls
            cos_b, sin_b = fine_ref[0, row : row + 1, :], fine_ref[1, row : row + 1, :]
            for part, value in enumerate(
                (cos_a * cos_b - sin_a * sin_b, sin_a * cos_b + cos_a * sin_b)
            ):
                high, low = split(value)
                rows = pl.ds((part * 2 + half) * blocks, blocks)
                high_ref[cls, rows, :] = high
                low_ref[cls, rows, :] = low


def depth_tables(depth_len, blocks):
    coarse, fine = depth_seeds(depth_len, blocks)
    shape = jax.ShapeDtypeStruct((4, 4 * blocks, depth_len // 4), BF16)
    return pl.pallas_call(
        table_kernel,
        out_shape=(shape, shape),
        in_specs=[VMEM, VMEM],
        out_specs=(VMEM, VMEM),
        compiler_params=pltpu.CompilerParams(vmem_limit_bytes=GRANT),
        name="depth_tables",
        cost_estimate=pl.CostEstimate(flops=10_000_000, bytes_accessed=5_000_000, transcendentals=0),
    )(coarse, fine)


def depth_forward_kernel(first, column, me_ref, own_ref, one_ref, two_ref, three_ref, high_ref, low_ref, *refs):
    rows, cells = own_ref.shape
    blocks = high_ref.shape[1] // 4
    cols = pl.ds(column, cells)
    me = me_ref[0]
    swap = (me & 1) == 1
    tau = (1 - 2 * (me & 1)).astype(F32)
    sigma = (1 - (me & 2)).astype(F32)
    even, odd = own_ref[...] + two_ref[...], one_ref[...] + three_ref[...]
    left, right = sigma * (own_ref[...] - two_ref[...]), sigma * (one_ref[...] - three_ref[...])
    both = jnp.concatenate(
        [jnp.where(swap, right, left), jnp.where(swap, left, right)], axis=0
    )

    def put(cls, real, imag):
        for plane, value in enumerate((real, imag)):
            for half in range(2):
                part = value[half * blocks : (half + 1) * blocks]
                slot = cls * 4 + plane * 2 + half
                if first:
                    refs[0][slot] = part
                else:
                    start = place_of(half * 4 + cls, plane)
                    refs[2][pl.ds(start, blocks, stride=16), :] = part + refs[0][slot]

    def send(side):
        if first:
            return []
        source = refs[2].reshape(blocks, 16, rows)
        tiles = pl.ds(side * 8, 8)
        save = pltpu.make_async_copy(source.at[:, tiles, :], refs[1].at[:, tiles, :], refs[3].at[side])
        save.start()
        return [save]

    def turn(cls, parts):
        return dot3((high_ref[cls, :, cols], low_ref[cls, :, cols]), parts, NT)

    top = 2 * blocks
    for cls, value in ((0, even + odd), (2, tau * (even - odd))):
        res = turn(cls, split(value))
        put(cls, res[:top], -res[top:])
    saves = send(0)
    parts = split(both)
    res = turn(1, parts)
    put(1, res[:top, :rows] - res[top:, rows:], -(res[top:, :rows] + res[:top, rows:]))
    res = turn(3, parts)
    put(3, res[:top, :rows] + res[top:, rows:], res[:top, rows:] - res[top:, :rows])
    for save in saves + send(1):
        save.wait()


def depth_forward(column, me, parts, tables, held=None):
    blocks = tables[0].shape[1] // 4
    rows = parts[0].shape[0]
    first = held is None
    shape = (16, blocks, rows) if first else (blocks, 16, rows)
    held_rows = [pltpu.VMEM((blocks * 16, rows), F32), pltpu.SemaphoreType.DMA((2,))]
    return pl.pallas_call(
        functools.partial(depth_forward_kernel, first, column),
        out_shape=jax.ShapeDtypeStruct(shape, F32) if first else pltpu.HBM(shape, F32),
        in_specs=[SMEM] + [VMEM] * (6 if first else 7),
        out_specs=VMEM if first else HBM,
        scratch_shapes=[] if first else held_rows,
        compiler_params=pltpu.CompilerParams(vmem_limit_bytes=GRANT),
        name="depth_forward",
        cost_estimate=pl.CostEstimate(flops=1_200_000_000, bytes_accessed=4_000_000, transcendentals=0),
    )(me, *parts, *tables, *(() if first else (held,)))


def depth_inverse_kernel(column, me_ref, y_ref, high_ref, low_ref, own_ref, one_ref, two_ref, three_ref):
    rows, cells = own_ref.shape
    blocks = high_ref.shape[1] // 4
    cols = pl.ds(column, cells)
    me = me_ref[0]
    swap = (me & 1) == 1
    tau = (1 - 2 * (me & 1)).astype(F32)
    sigma = (1 - (me & 2)).astype(F32)

    def get(cls, plane):
        value = jnp.concatenate(
            [y_ref[pl.ds(plane * 8 + half * 4 + cls, blocks, stride=16), :] for half in range(2)],
            axis=0,
        )
        if cls == 0:
            first = lax.broadcasted_iota(jnp.int32, value.shape, 0) == 0
            value = jnp.where(first, 0.5 * value, value)
        return split(value.T)

    def turn(cls, *lines):
        left = [
            jnp.concatenate([jnp.concatenate(line, axis=1) for line in part], axis=0)
            for part in zip(*[[(a, b) for a, b in zip(*line)] for line in lines])
        ]
        return dot3(left, (high_ref[cls, :, cols], low_ref[cls, :, cols]), NN)

    def minus(parts):
        return [-part for part in parts]

    real, imag = get(0, 0), get(0, 1)
    zero = turn(0, (real, minus(imag)))
    real, imag = get(2, 0), get(2, 1)
    two = tau * turn(2, (real, minus(imag)))
    real, imag = get(1, 0), get(1, 1)
    odd = turn(1, (real, minus(imag)), (minus(imag), minus(real)))
    real, imag = get(3, 0), get(3, 1)
    odd = sigma * (odd + turn(3, (real, minus(imag)), (imag, real)))
    low, high = odd[:rows], odd[rows:]
    base, turned = zero + two, jnp.where(swap, high, low)
    own_ref[...] = base + turned
    two_ref[...] = base - turned
    base, turned = zero - two, jnp.where(swap, low, high)
    one_ref[...] = base + turned
    three_ref[...] = base - turned


def depth_inverse(column, width, me, waves, tables):
    rows = waves.shape[1]
    shape = jax.ShapeDtypeStruct((rows, width), F32)
    return pl.pallas_call(
        functools.partial(depth_inverse_kernel, column),
        out_shape=(shape,) * 4,
        in_specs=[SMEM] + [VMEM] * 3,
        out_specs=(VMEM,) * 4,
        compiler_params=pltpu.CompilerParams(vmem_limit_bytes=GRANT),
        name="depth_inverse",
        cost_estimate=pl.CostEstimate(flops=1_200_000_000, bytes_accessed=4_000_000, transcendentals=0),
    )(me, waves, *tables)


def strike_tables(edge, scale):
    turn = 2.0 * np.pi / edge
    angle = turn * (np.outer(np.arange(edge), np.arange(edge)) % edge)
    waves = np.stack([*split_np(np.cos(angle)), *split_np(np.sin(angle))])
    twist = 2.0 * np.pi / (edge * edge) * np.outer(np.arange(edge), np.arange(edge))
    twist = np.stack([np.cos(twist), np.sin(twist)]) * scale
    return waves, np.concatenate([twist, 2.0 * twist]).astype(np.float32)


def strike_kernel(
    x_ref, gain_hbm, past_hbm, wave_ref, twist_ref, modes_hbm, out_ref,
    gain_ref, past_ref, held_ref, modes_ref, sems,
):
    edge = twist_ref.shape[1]
    pairs = ((gain_hbm, gain_ref), (past_hbm, past_ref))
    loads = [pltpu.make_async_copy(a, b, sems.at[n]) for n, (a, b) in enumerate(pairs)]
    for load in loads:
        load.start()

    def lines(group):
        return range(group * PAIR, (group + 1) * PAIR)

    def lanes(value, place):
        part = value[:, place * edge : (place + 1) * edge]
        return part[:edge], part[edge:]

    def gather(m):
        return jnp.concatenate(
            [x_ref[pl.ds(place_of(m, plane), edge, stride=16), :] for plane in range(2)], axis=0
        )

    def block(sign, part):
        cosine, sine = wave_ref[part], wave_ref[2 + part]
        left, right = (sine, -sine) if sign > 0 else (-sine, sine)
        return jnp.concatenate(
            [jnp.concatenate([cosine, left], axis=1), jnp.concatenate([right, cosine], axis=1)], axis=0
        )

    def rotate(value, sign, cosine, sine):
        rows = []
        for place in range(PAIR):
            real, imag = lanes(value, place)
            if sign > 0:
                rows.append([real * cosine + imag * sine, imag * cosine - real * sine])
            else:
                rows.append([real * cosine - imag * sine, imag * cosine + real * sine])
        return jnp.concatenate([jnp.concatenate(row, axis=1) for row in rows], axis=0)

    groups = 8 // PAIR
    forward = (block(1, 0), block(1, 1))
    kept = None
    for group in range(groups + 1):
        before, kept = kept, None
        if group < groups:
            value = jnp.concatenate([gather(m) for m in lines(group)], axis=1)
            kept = dot3(forward, split(value), NN)
        if group > 0:
            value = dot3(forward, split(rotate(before, 1, twist_ref[0], twist_ref[1])), NT)
            for place, m in enumerate(lines(group - 1)):
                for plane, part in enumerate(lanes(value, place)):
                    held_ref[plane, m] = part
                    modes_ref[plane, pl.ds(m, edge, stride=8), :] = part
    save = pltpu.make_async_copy(modes_ref, modes_hbm, sems.at[2])
    save.start()
    for load in loads:
        load.wait()
    backward = (block(-1, 0), block(-1, 1))
    for group in range(groups + 1):
        before, kept = kept, None
        if group < groups:
            value = jnp.concatenate(
                [
                    jnp.concatenate(
                        [
                            gain_ref[m] * held_ref[plane, m] + past_ref[plane, m]
                            for plane in range(2)
                        ],
                        axis=0,
                    )
                    for m in lines(group)
                ],
                axis=1,
            )
            kept = dot3(backward, split(value), NN)
        if group > 0:
            value = dot3(backward, split(rotate(before, -1, twist_ref[2], twist_ref[3])), NT)
            for place, m in enumerate(lines(group - 1)):
                for plane, part in enumerate(lanes(value, place)):
                    out_ref[pl.ds(plane * 8 + m, edge, stride=16), :] = part
    save.wait()


def strike_both(pencil, gain, past, tables):
    waves, twist = tables
    edge = twist.shape[1]
    modes = (2, edge * 8, edge)
    return pl.pallas_call(
        strike_kernel,
        out_shape=(
            pltpu.HBM(modes, F32),
            jax.ShapeDtypeStruct((edge * 16, edge), F32),
        ),
        in_specs=[VMEM, HBM, HBM, VMEM, VMEM],
        out_specs=(HBM, VMEM),
        scratch_shapes=[
            pltpu.VMEM(gain.shape, F32),
            pltpu.VMEM(past.shape, F32),
            pltpu.VMEM(past.shape, F32),
            pltpu.VMEM(modes, F32),
            pltpu.SemaphoreType.DMA((3,)),
        ],
        compiler_params=pltpu.CompilerParams(vmem_limit_bytes=WIDE),
        name="strike_both",
        cost_estimate=pl.CostEstimate(flops=1_600_000_000, bytes_accessed=6_000_000, transcendentals=0),
    )(pencil, *in_hbm(gain, past), waves, twist)


def past_kernel(kernel_ref, history_ref, gain_ref, past_ref):
    for tile in range(kernel_ref.shape[2] // 128):
        cols = pl.ds(tile * 128, 128)
        gain_ref[:, tile, :] = kernel_ref[0, :, cols]
        for plane in range(2):
            total = kernel_ref[1, :, cols] * history_ref[0, plane, :, cols]
            for lag in range(1, LAGS):
                total = total + kernel_ref[lag + 1, :, cols] * history_ref[lag, plane, :, cols]
            past_ref[plane, :, tile, :] = total


def past_sum(kernel, history):
    length = kernel.shape[2]
    block = 2048
    return pl.pallas_call(
        past_kernel,
        grid=(length // block,),
        out_shape=(
            pltpu.HBM((8, length // 128, 128), F32),
            pltpu.HBM((2, 8, length // 128, 128), F32),
        ),
        in_specs=[
            pl.BlockSpec((LAGS + 1, 8, block), lambda i: (0, 0, i)),
            pl.BlockSpec((LAGS, 2, 8, block), lambda i: (0, 0, 0, i)),
        ],
        out_specs=(
            pl.BlockSpec((8, block // 128, 128), lambda i: (0, i, 0)),
            pl.BlockSpec((2, 8, block // 128, 128), lambda i: (0, 0, i, 0)),
        ),
        compiler_params=pltpu.CompilerParams(vmem_limit_bytes=WIDE),
        name="past_sum",
        cost_estimate=pl.CostEstimate(flops=4_200_000, bytes_accessed=14_700_000, transcendentals=0),
    )(*in_hbm(kernel, history))


def newton_parts(rate, scaling, strength):
    scaled = rate * scaling
    magnitude = jnp.abs(scaled)
    square = 1.0 + scaled * scaled
    inverse = lax.rsqrt(square)
    positive = jnp.log(magnitude + square * inverse)
    friction = strength * jnp.where(scaled < 0, -positive, positive)
    return friction, 1.0 + (strength * scaling) * (inverse * (1.0 / DAMPING))


STEP = RELAXATION / DAMPING


def start_kernel(rate_ref, state_ref, weak_ref, strength_ref, stress_ref, scale_ref, rest_ref, gain_ref):
    scaling = 0.5 * jnp.exp(weak_ref[...] * state_ref[...])
    rate = rate_ref[...]
    friction, divisor = newton_parts(rate, scaling, strength_ref[...])
    gain = STEP / divisor
    scale_ref[...] = scaling
    gain_ref[...] = gain
    rest_ref[...] = rate + gain * (stress_ref[...] - DAMPING * rate - friction)


def friction_start(rate_prev, log_state, weakening, strength, pre_stress):
    rows, cells = rate_prev.shape
    spec = pl.BlockSpec((64, cells), lambda i: (i, 0))
    shape = jax.ShapeDtypeStruct((rows, cells), F32)
    return pl.pallas_call(
        start_kernel,
        grid=(rows // 64,),
        out_shape=(shape,) * 3,
        in_specs=[spec] * 5,
        out_specs=(spec,) * 3,
        compiler_params=pltpu.CompilerParams(vmem_limit_bytes=GRANT),
        name="friction_start",
        cost_estimate=pl.CostEstimate(flops=20_000_000, bytes_accessed=8_000_000, transcendentals=1_000_000),
    )(rate_prev, log_state, weakening, strength, pre_stress)


def friction_kernel(
    slots, column, me_ref, scale_ref, rest_ref, gain_ref, strength_ref, stress_ref, slip_ref, *refs
):
    velocity_hbm, new_hbm, velocity_ref, new_ref, sems = refs[-5:]
    parts = refs[: len(slots)]
    edge, width = parts[0].shape
    cols = pl.ds(column, width)
    saves = []
    for place, (slot, ref) in enumerate(zip(slots, parts)):
        rows = pl.ds(pl.multiple_of((me_ref[0] ^ slot) * edge, edge), edge)
        elastic = ref[...]
        scaling, strength = scale_ref[rows, cols], strength_ref[rows, cols]
        total = stress_ref[rows, cols] + elastic
        rate = rest_ref[rows, cols] + gain_ref[rows, cols] * elastic
        for sweep in range(NEWTON_ITERS - 1):
            friction, divisor = newton_parts(rate, scaling, strength)
            rate = rate + STEP * (total - DAMPING * rate - friction) / divisor
        velocity_ref[place] = rate
        new_ref[place] = slip_ref[rows, cols] + ADVANCE * rate
        for n, (source, target) in enumerate(((velocity_ref, velocity_hbm), (new_ref, new_hbm))):
            save = pltpu.make_async_copy(source.at[place], target.at[rows, cols], sems.at[place, n])
            save.start()
            saves.append(save)
    for save in saves:
        save.wait()


def friction_finish(slots, column, me, elastic, start, strength, pre_stress, fault_slip, held=()):
    edge, width = elastic[0].shape
    shape = jax.ShapeDtypeStruct(fault_slip.shape, F32)
    count = 7 + len(slots)
    return pl.pallas_call(
        functools.partial(friction_kernel, slots, column),
        in_specs=[SMEM] + [VMEM] * (6 + len(slots)) + [HBM] * len(held),
        out_specs=(HBM, HBM),
        out_shape=(shape, shape),
        scratch_shapes=[
            pltpu.VMEM((len(slots), edge, width), F32),
            pltpu.VMEM((len(slots), edge, width), F32),
            pltpu.SemaphoreType.DMA((len(slots), 2)),
        ],
        input_output_aliases={count + n: n for n in range(len(held))},
        compiler_params=pltpu.CompilerParams(vmem_limit_bytes=GRANT),
        name="friction_finish",
        cost_estimate=pl.CostEstimate(flops=20_000_000, bytes_accessed=5_000_000, transcendentals=1_000_000),
    )(me, *start, strength, pre_stress, fault_slip, *elastic, *in_hbm(*held))


def exchange(parts, size):
    swap = lambda part, k: lax.ppermute(part, "depth", [(place, place ^ k) for place in range(size)])
    moved = {k: swap(parts[k], k) for k in (2, 3, 1)}
    return [parts[0]] + [moved[k] for k in (1, 2, 3)]


def body(fault_slip, rate_prev, log_state, weakening, strength, pre_stress, kernel, history):
    rows, cells = fault_slip.shape
    depth_size = lax.axis_size("depth")
    devices = lax.axis_size("strike") * depth_size
    edge = rows // depth_size
    depth_len = cells * depth_size
    place = lax.axis_index("depth")
    me = place.reshape(1)
    block = lambda source, k, part: lax.dynamic_slice(
        source, ((place ^ k) * edge, part[0]), (edge, part[1])
    )
    far = [block(fault_slip, k, FORWARD[0]) for k in (2, 3)]
    source, *far = lax.optimization_barrier((fault_slip, *far))
    near = [block(source, k, FORWARD[0]) for k in (0, 1)]
    lines = [exchange(near + far, depth_size)]
    for part in FORWARD[1:]:
        lines.append(exchange([block(source, k, part) for k in range(depth_size)], depth_size))
    tables = depth_tables(depth_len, devices)
    gain, past = past_sum(kernel, history)
    waves = None
    for (column, _), parts in zip(FORWARD, lines):
        waves = depth_forward(column, me, parts, tables, waves)
    pencil = lax.all_to_all(waves, ALL, 0, 0)
    scale = 1.0 / math.sqrt(depth_len * edge * devices)
    modes, waves = strike_both(
        pencil.reshape(devices * 16, edge), gain, past, strike_tables(edge, scale)
    )
    start = friction_start(rate_prev, log_state, weakening, strength, pre_stress)
    waves = lax.all_to_all(waves.reshape(devices, 16, edge), ALL, 0, 0).reshape(devices * 16, edge)
    elastic = [
        exchange(depth_inverse(column, width, me, waves, tables), depth_size)
        for column, width in INVERSE
    ]
    out = ()
    for (column, _), parts, groups in zip(INVERSE, elastic, SLOTS):
        for slots in groups:
            parts_now = [parts[slot] for slot in slots]
            out = friction_finish(
                slots, column, me, parts_now, start, strength, pre_stress, fault_slip, out
            )
    slip_modes = modes.reshape(2, devices, 8, edge).transpose(0, 2, 1, 3).reshape(2, 8, devices * edge)
    return (*out, slip_modes)


def solution(mesh):
    return jax.shard_map(
        body,
        mesh=mesh,
        in_specs=(
            P("strike", "depth"),
            P("strike", "depth"),
            P("strike", "depth"),
            P("strike", "depth"),
            P("strike", "depth"),
            P("strike", "depth"),
            P(None, ("strike", "depth"), None),
            P(None, None, ("strike", "depth"), None),
        ),
        out_specs=(P("strike", "depth"), P("strike", "depth"), P(None, ("strike", "depth"), None)),
        check_vma=False,
    )
```

```python
import functools
import math

import jax
import jax.numpy as jnp
import ml_dtypes
import numpy as np
from jax import lax
from jax.experimental import pallas as pl
from jax.experimental.pallas import tpu as pltpu
from jax.sharding import PartitionSpec as P

NEWTON_ITERS = 4
DAMPING = 0.5
RELAXATION = 0.5
ADVANCE = 0.5
LAGS = 8
FORWARD = ((0, 384), (384, 128))
INVERSE = ((0, 256), (256, 256))
SLOTS = (((0, 1, 2, 3),), ((0, 1), (2,), (3,)))
PAIR = 2
GRANT = 16 << 20
WIDE = 24 << 20
ALL = ("strike", "depth")
F32 = jnp.float32
BF16 = jnp.bfloat16
NN = (((1,), (0,)), ((), ()))
NT = (((1,), (1,)), ((), ()))
TN = (((0,), (0,)), ((), ()))
VMEM = pl.BlockSpec(memory_space=pltpu.VMEM)
SMEM = pl.BlockSpec(memory_space=pltpu.SMEM)
HBM = pl.BlockSpec(memory_space=pltpu.HBM)


def split_np(table):
    high = table.astype(ml_dtypes.bfloat16)
    low = (table - high.astype(np.float64)).astype(ml_dtypes.bfloat16)
    return high, low


def split(value):
    high = value.astype(BF16)
    return high, (value - high.astype(F32)).astype(BF16)


def in_hbm(*values):
    return [pltpu.with_memory_space_constraint(jnp.asarray(v), pltpu.HBM) for v in values]


def dot3(left, right, dims):
    (left_axis,), (right_axis,) = dims[0]
    return lax.dot_general(
        jnp.concatenate([left[0], left[0], left[1]], axis=left_axis),
        jnp.concatenate([right[0], right[1], right[0]], axis=right_axis),
        dims,
        preferred_element_type=F32,
    )


def place_of(mode, plane):
    half, cls = divmod(mode, 4)
    return (cls % 2) * 8 + plane * 4 + half * 2 + cls // 2


def depth_seeds(depth_len, blocks):
    cells = depth_len // 4
    cell = np.arange(cells)
    turn = 2.0 * np.pi / depth_len
    coarse = turn * ((8 * np.arange(blocks)[:, None] * cell[None]) % depth_len)
    fine = turn * ((np.arange(8)[:, None] * cell[None]) % depth_len)
    pack = lambda angle: np.stack([np.cos(angle), np.sin(angle)]).astype(np.float32)
    return pack(coarse), pack(fine)


def table_kernel(coarse_ref, fine_ref, high_ref, low_ref):
    blocks = coarse_ref.shape[1]
    cos_a, sin_a = coarse_ref[0], coarse_ref[1]
    for cls in range(4):
        for half in range(2):
            row = 4 * half + cls
            cos_b, sin_b = fine_ref[0, row : row + 1, :], fine_ref[1, row : row + 1, :]
            for part, value in enumerate(
                (cos_a * cos_b - sin_a * sin_b, sin_a * cos_b + cos_a * sin_b)
            ):
                high, low = split(value)
                rows = pl.ds((part * 2 + half) * blocks, blocks)
                high_ref[cls, rows, :] = high
                low_ref[cls, rows, :] = low


def depth_tables(depth_len, blocks):
    coarse, fine = depth_seeds(depth_len, blocks)
    shape = jax.ShapeDtypeStruct((4, 4 * blocks, depth_len // 4), BF16)
    return pl.pallas_call(
        table_kernel,
        out_shape=(shape, shape),
        in_specs=[VMEM, VMEM],
        out_specs=(VMEM, VMEM),
        compiler_params=pltpu.CompilerParams(vmem_limit_bytes=GRANT),
        name="depth_tables",
        cost_estimate=pl.CostEstimate(flops=10_000_000, bytes_accessed=5_000_000, transcendentals=0),
    )(coarse, fine)


def depth_forward_kernel(first, column, me_ref, own_ref, one_ref, two_ref, three_ref, high_ref, low_ref, *refs):
    rows, cells = own_ref.shape
    blocks = high_ref.shape[1] // 4
    cols = pl.ds(column, cells)
    me = me_ref[0]
    swap = (me & 1) == 1
    tau = (1 - 2 * (me & 1)).astype(F32)
    sigma = (1 - (me & 2)).astype(F32)
    even, odd = own_ref[...] + two_ref[...], one_ref[...] + three_ref[...]
    left, right = sigma * (own_ref[...] - two_ref[...]), sigma * (one_ref[...] - three_ref[...])
    both = jnp.concatenate(
        [jnp.where(swap, right, left), jnp.where(swap, left, right)], axis=0
    )

    def put(cls, real, imag):
        for plane, value in enumerate((real, imag)):
            for half in range(2):
                part = value[half * blocks : (half + 1) * blocks]
                slot = cls * 4 + plane * 2 + half
                if first:
                    refs[0][slot] = part
                else:
                    start = place_of(half * 4 + cls, plane)
                    refs[2][pl.ds(start, blocks, stride=16), :] = part + refs[0][slot]

    def send(side):
        if first:
            return []
        source = refs[2].reshape(blocks, 16, rows)
        tiles = pl.ds(side * 8, 8)
        save = pltpu.make_async_copy(source.at[:, tiles, :], refs[1].at[:, tiles, :], refs[3].at[side])
        save.start()
        return [save]

    def turn(cls, parts):
        return dot3((high_ref[cls, :, cols], low_ref[cls, :, cols]), parts, NT)

    top = 2 * blocks
    for cls, value in ((0, even + odd), (2, tau * (even - odd))):
        res = turn(cls, split(value))
        put(cls, res[:top], -res[top:])
    saves = send(0)
    parts = split(both)
    res = turn(1, parts)
    put(1, res[:top, :rows] - res[top:, rows:], -(res[top:, :rows] + res[:top, rows:]))
    res = turn(3, parts)
    put(3, res[:top, :rows] + res[top:, rows:], res[:top, rows:] - res[top:, :rows])
    for save in saves + send(1):
        save.wait()


def depth_forward(column, me, parts, tables, held=None):
    blocks = tables[0].shape[1] // 4
    rows = parts[0].shape[0]
    first = held is None
    shape = (16, blocks, rows) if first else (blocks, 16, rows)
    held_rows = [pltpu.VMEM((blocks * 16, rows), F32), pltpu.SemaphoreType.DMA((2,))]
    return pl.pallas_call(
        functools.partial(depth_forward_kernel, first, column),
        out_shape=jax.ShapeDtypeStruct(shape, F32) if first else pltpu.HBM(shape, F32),
        in_specs=[SMEM] + [VMEM] * (6 if first else 7),
        out_specs=VMEM if first else HBM,
        scratch_shapes=[] if first else held_rows,
        compiler_params=pltpu.CompilerParams(vmem_limit_bytes=GRANT),
        name="depth_forward",
        cost_estimate=pl.CostEstimate(flops=1_200_000_000, bytes_accessed=4_000_000, transcendentals=0),
    )(me, *parts, *tables, *(() if first else (held,)))


def depth_inverse_kernel(column, me_ref, y_ref, high_ref, low_ref, own_ref, one_ref, two_ref, three_ref):
    rows, cells = own_ref.shape
    blocks = high_ref.shape[1] // 4
    cols = pl.ds(column, cells)
    me = me_ref[0]
    swap = (me & 1) == 1
    tau = (1 - 2 * (me & 1)).astype(F32)
    sigma = (1 - (me & 2)).astype(F32)

    def get(cls, plane):
        value = jnp.concatenate(
            [y_ref[pl.ds(plane * 8 + half * 4 + cls, blocks, stride=16), :] for half in range(2)],
            axis=0,
        )
        if cls == 0:
            first = lax.broadcasted_iota(jnp.int32, value.shape, 0) == 0
            value = jnp.where(first, 0.5 * value, value)
        return split(value.T)

    def stack(*lines):
        return [
            jnp.concatenate([jnp.concatenate(line, axis=1) for line in part], axis=0)
            for part in zip(*[[(a, b) for a, b in zip(*line)] for line in lines])
        ]

    def turn(classes, lefts):
        left = [jnp.concatenate(part, axis=1) for part in zip(*lefts)]
        table = [
            jnp.concatenate([ref[cls, :, cols] for cls in classes], axis=0)
            for ref in (high_ref, low_ref)
        ]
        return dot3(left, table, NN)

    def minus(parts):
        return [-part for part in parts]

    real, imag = get(0, 0), get(0, 1)
    zero = turn((0,), [stack((real, minus(imag)))])
    real, imag = get(2, 0), get(2, 1)
    two = tau * turn((2,), [stack((real, minus(imag)))])
    real, imag = get(1, 0), get(1, 1)
    odd = stack((real, minus(imag)), (minus(imag), minus(real)))
    real, imag = get(3, 0), get(3, 1)
    odd = sigma * turn((1, 3), [odd, stack((real, minus(imag)), (imag, real))])
    low, high = odd[:rows], odd[rows:]
    base, turned = zero + two, jnp.where(swap, high, low)
    own_ref[...] = base + turned
    two_ref[...] = base - turned
    base, turned = zero - two, jnp.where(swap, low, high)
    one_ref[...] = base + turned
    three_ref[...] = base - turned


def depth_inverse(column, width, me, waves, tables):
    rows = waves.shape[1]
    shape = jax.ShapeDtypeStruct((rows, width), F32)
    return pl.pallas_call(
        functools.partial(depth_inverse_kernel, column),
        out_shape=(shape,) * 4,
        in_specs=[SMEM] + [VMEM] * 3,
        out_specs=(VMEM,) * 4,
        compiler_params=pltpu.CompilerParams(vmem_limit_bytes=GRANT),
        name="depth_inverse",
        cost_estimate=pl.CostEstimate(flops=1_200_000_000, bytes_accessed=4_000_000, transcendentals=0),
    )(me, waves, *tables)


def strike_tables(edge, scale):
    turn = 2.0 * np.pi / edge
    angle = turn * (np.outer(np.arange(edge), np.arange(edge)) % edge)
    waves = np.stack([*split_np(np.cos(angle)), *split_np(np.sin(angle))])
    twist = 2.0 * np.pi / (edge * edge) * np.outer(np.arange(edge), np.arange(edge))
    twist = np.stack([np.cos(twist), np.sin(twist)]) * scale
    return waves, np.concatenate([twist, 2.0 * twist]).astype(np.float32)


def strike_kernel(
    x_ref, gain_hbm, past_hbm, wave_ref, twist_ref, modes_hbm, out_ref,
    gain_ref, past_ref, held_ref, modes_ref, sems,
):
    edge = twist_ref.shape[1]
    pairs = ((gain_hbm, gain_ref), (past_hbm, past_ref))
    loads = [pltpu.make_async_copy(a, b, sems.at[n]) for n, (a, b) in enumerate(pairs)]
    for load in loads:
        load.start()

    def lines(group):
        return range(group * PAIR, (group + 1) * PAIR)

    def lanes(value, place):
        part = value[:, place * edge : (place + 1) * edge]
        return part[:edge], part[edge:]

    def gather(m):
        return jnp.concatenate(
            [x_ref[pl.ds(place_of(m, plane), edge, stride=16), :] for plane in range(2)], axis=0
        )

    def block(sign, part):
        cosine, sine = wave_ref[part], wave_ref[2 + part]
        left, right = (sine, -sine) if sign > 0 else (-sine, sine)
        return jnp.concatenate(
            [jnp.concatenate([cosine, left], axis=1), jnp.concatenate([right, cosine], axis=1)], axis=0
        )

    def rotate(value, sign, cosine, sine):
        rows = []
        for place in range(PAIR):
            real, imag = lanes(value, place)
            if sign > 0:
                rows.append([real * cosine + imag * sine, imag * cosine - real * sine])
            else:
                rows.append([real * cosine - imag * sine, imag * cosine + real * sine])
        return jnp.concatenate([jnp.concatenate(row, axis=1) for row in rows], axis=0)

    groups = 8 // PAIR
    forward = (block(1, 0), block(1, 1))
    kept = None
    for group in range(groups + 1):
        before, kept = kept, None
        if group < groups:
            value = jnp.concatenate([gather(m) for m in lines(group)], axis=1)
            kept = dot3(forward, split(value), NN)
        if group > 0:
            value = dot3(forward, split(rotate(before, 1, twist_ref[0], twist_ref[1])), NT)
            for place, m in enumerate(lines(group - 1)):
                for plane, part in enumerate(lanes(value, place)):
                    held_ref[plane, m] = part
                    modes_ref[plane, pl.ds(m, edge, stride=8), :] = part
    save = pltpu.make_async_copy(modes_ref, modes_hbm, sems.at[2])
    save.start()
    for load in loads:
        load.wait()
    backward = (block(-1, 0), block(-1, 1))
    for group in range(groups + 1):
        before, kept = kept, None
        if group < groups:
            value = jnp.concatenate(
                [
                    jnp.concatenate(
                        [
                            gain_ref[m] * held_ref[plane, m] + past_ref[plane, m]
                            for plane in range(2)
                        ],
                        axis=0,
                    )
                    for m in lines(group)
                ],
                axis=1,
            )
            kept = dot3(backward, split(value), NN)
        if group > 0:
            value = dot3(backward, split(rotate(before, -1, twist_ref[2], twist_ref[3])), NT)
            for place, m in enumerate(lines(group - 1)):
                for plane, part in enumerate(lanes(value, place)):
                    out_ref[pl.ds(plane * 8 + m, edge, stride=16), :] = part
    save.wait()


def strike_both(pencil, gain, past, tables):
    waves, twist = tables
    edge = twist.shape[1]
    modes = (2, edge * 8, edge)
    return pl.pallas_call(
        strike_kernel,
        out_shape=(
            pltpu.HBM(modes, F32),
            jax.ShapeDtypeStruct((edge * 16, edge), F32),
        ),
        in_specs=[VMEM, HBM, HBM, VMEM, VMEM],
        out_specs=(HBM, VMEM),
        scratch_shapes=[
            pltpu.VMEM(gain.shape, F32),
            pltpu.VMEM(past.shape, F32),
            pltpu.VMEM(past.shape, F32),
            pltpu.VMEM(modes, F32),
            pltpu.SemaphoreType.DMA((3,)),
        ],
        compiler_params=pltpu.CompilerParams(vmem_limit_bytes=WIDE),
        name="strike_both",
        cost_estimate=pl.CostEstimate(flops=1_600_000_000, bytes_accessed=6_000_000, transcendentals=0),
    )(pencil, *in_hbm(gain, past), waves, twist)


def past_kernel(kernel_ref, history_ref, gain_ref, past_ref):
    for tile in range(kernel_ref.shape[2] // 128):
        cols = pl.ds(tile * 128, 128)
        gain_ref[:, tile, :] = kernel_ref[0, :, cols]
        for plane in range(2):
            total = kernel_ref[1, :, cols] * history_ref[0, plane, :, cols]
            for lag in range(1, LAGS):
                total = total + kernel_ref[lag + 1, :, cols] * history_ref[lag, plane, :, cols]
            past_ref[plane, :, tile, :] = total


def past_sum(kernel, history):
    length = kernel.shape[2]
    block = 2048
    return pl.pallas_call(
        past_kernel,
        grid=(length // block,),
        out_shape=(
            pltpu.HBM((8, length // 128, 128), F32),
            pltpu.HBM((2, 8, length // 128, 128), F32),
        ),
        in_specs=[
            pl.BlockSpec((LAGS + 1, 8, block), lambda i: (0, 0, i)),
            pl.BlockSpec((LAGS, 2, 8, block), lambda i: (0, 0, 0, i)),
        ],
        out_specs=(
            pl.BlockSpec((8, block // 128, 128), lambda i: (0, i, 0)),
            pl.BlockSpec((2, 8, block // 128, 128), lambda i: (0, 0, i, 0)),
        ),
        compiler_params=pltpu.CompilerParams(vmem_limit_bytes=WIDE),
        name="past_sum",
        cost_estimate=pl.CostEstimate(flops=4_200_000, bytes_accessed=14_700_000, transcendentals=0),
    )(*in_hbm(kernel, history))


def newton_parts(rate, scaling, strength):
    scaled = rate * scaling
    magnitude = jnp.abs(scaled)
    square = 1.0 + scaled * scaled
    inverse = lax.rsqrt(square)
    positive = jnp.log(magnitude + square * inverse)
    friction = strength * jnp.where(scaled < 0, -positive, positive)
    return friction, 1.0 + (strength * scaling) * (inverse * (1.0 / DAMPING))


STEP = RELAXATION / DAMPING


def start_kernel(rate_ref, state_ref, weak_ref, strength_ref, stress_ref, scale_ref, rest_ref, gain_ref):
    scaling = 0.5 * jnp.exp(weak_ref[...] * state_ref[...])
    rate = rate_ref[...]
    friction, divisor = newton_parts(rate, scaling, strength_ref[...])
    gain = STEP / divisor
    scale_ref[...] = scaling
    gain_ref[...] = gain
    rest_ref[...] = rate + gain * (stress_ref[...] - DAMPING * rate - friction)


def friction_start(rate_prev, log_state, weakening, strength, pre_stress):
    rows, cells = rate_prev.shape
    spec = pl.BlockSpec((64, cells), lambda i: (i, 0))
    shape = jax.ShapeDtypeStruct((rows, cells), F32)
    return pl.pallas_call(
        start_kernel,
        grid=(rows // 64,),
        out_shape=(shape,) * 3,
        in_specs=[spec] * 5,
        out_specs=(spec,) * 3,
        compiler_params=pltpu.CompilerParams(vmem_limit_bytes=GRANT),
        name="friction_start",
        cost_estimate=pl.CostEstimate(flops=20_000_000, bytes_accessed=8_000_000, transcendentals=1_000_000),
    )(rate_prev, log_state, weakening, strength, pre_stress)


def friction_kernel(
    slots, column, me_ref, scale_ref, rest_ref, gain_ref, strength_ref, stress_ref, slip_ref, *refs
):
    velocity_hbm, new_hbm, velocity_ref, new_ref, sems = refs[-5:]
    parts = refs[: len(slots)]
    edge, width = parts[0].shape
    cols = pl.ds(column, width)
    saves = []
    for place, (slot, ref) in enumerate(zip(slots, parts)):
        rows = pl.ds(pl.multiple_of((me_ref[0] ^ slot) * edge, edge), edge)
        elastic = ref[...]
        scaling, strength = scale_ref[rows, cols], strength_ref[rows, cols]
        total = stress_ref[rows, cols] + elastic
        rate = rest_ref[rows, cols] + gain_ref[rows, cols] * elastic
        for sweep in range(NEWTON_ITERS - 1):
            friction, divisor = newton_parts(rate, scaling, strength)
            rate = rate + STEP * (total - DAMPING * rate - friction) / divisor
        velocity_ref[place] = rate
        new_ref[place] = slip_ref[rows, cols] + ADVANCE * rate
        for n, (source, target) in enumerate(((velocity_ref, velocity_hbm), (new_ref, new_hbm))):
            save = pltpu.make_async_copy(source.at[place], target.at[rows, cols], sems.at[place, n])
            save.start()
            saves.append(save)
    for save in saves:
        save.wait()


def friction_finish(slots, column, me, elastic, start, strength, pre_stress, fault_slip, held=()):
    edge, width = elastic[0].shape
    shape = jax.ShapeDtypeStruct(fault_slip.shape, F32)
    count = 7 + len(slots)
    return pl.pallas_call(
        functools.partial(friction_kernel, slots, column),
        in_specs=[SMEM] + [VMEM] * (6 + len(slots)) + [HBM] * len(held),
        out_specs=(HBM, HBM),
        out_shape=(shape, shape),
        scratch_shapes=[
            pltpu.VMEM((len(slots), edge, width), F32),
            pltpu.VMEM((len(slots), edge, width), F32),
            pltpu.SemaphoreType.DMA((len(slots), 2)),
        ],
        input_output_aliases={count + n: n for n in range(len(held))},
        compiler_params=pltpu.CompilerParams(vmem_limit_bytes=GRANT),
        name="friction_finish",
        cost_estimate=pl.CostEstimate(flops=20_000_000, bytes_accessed=5_000_000, transcendentals=1_000_000),
    )(me, *start, strength, pre_stress, fault_slip, *elastic, *in_hbm(*held))


def exchange(parts, size):
    swap = lambda part, k: lax.ppermute(part, "depth", [(place, place ^ k) for place in range(size)])
    moved = {k: swap(parts[k], k) for k in (2, 3, 1)}
    return [parts[0]] + [moved[k] for k in (1, 2, 3)]


def body(fault_slip, rate_prev, log_state, weakening, strength, pre_stress, kernel, history):
    rows, cells = fault_slip.shape
    depth_size = lax.axis_size("depth")
    devices = lax.axis_size("strike") * depth_size
    edge = rows // depth_size
    depth_len = cells * depth_size
    place = lax.axis_index("depth")
    me = place.reshape(1)
    block = lambda source, k, part: lax.dynamic_slice(
        source, ((place ^ k) * edge, part[0]), (edge, part[1])
    )
    far = [block(fault_slip, k, FORWARD[0]) for k in (2, 3)]
    source, *far = lax.optimization_barrier((fault_slip, *far))
    near = [block(source, k, FORWARD[0]) for k in (0, 1)]
    lines = [exchange(near + far, depth_size)]
    for part in FORWARD[1:]:
        lines.append(exchange([block(source, k, part) for k in range(depth_size)], depth_size))
    tables = depth_tables(depth_len, devices)
    gain, past = past_sum(kernel, history)
    waves = None
    for (column, _), parts in zip(FORWARD, lines):
        waves = depth_forward(column, me, parts, tables, waves)
    pencil = lax.all_to_all(waves, ALL, 0, 0)
    scale = 1.0 / math.sqrt(depth_len * edge * devices)
    modes, waves = strike_both(
        pencil.reshape(devices * 16, edge), gain, past, strike_tables(edge, scale)
    )
    start = friction_start(rate_prev, log_state, weakening, strength, pre_stress)
    waves = lax.all_to_all(waves.reshape(devices, 16, edge), ALL, 0, 0).reshape(devices * 16, edge)
    elastic = [
        exchange(depth_inverse(column, width, me, waves, tables), depth_size)
        for column, width in INVERSE
    ]
    out = ()
    for (column, _), parts, groups in zip(INVERSE, elastic, SLOTS):
        for slots in groups:
            parts_now = [parts[slot] for slot in slots]
            out = friction_finish(
                slots, column, me, parts_now, start, strength, pre_stress, fault_slip, out
            )
    slip_modes = modes.reshape(2, devices, 8, edge).transpose(0, 2, 1, 3).reshape(2, 8, devices * edge)
    return (*out, slip_modes)


def solution(mesh):
    return jax.shard_map(
        body,
        mesh=mesh,
        in_specs=(
            P("strike", "depth"),
            P("strike", "depth"),
            P("strike", "depth"),
            P("strike", "depth"),
            P("strike", "depth"),
            P("strike", "depth"),
            P(None, ("strike", "depth"), None),
            P(None, None, ("strike", "depth"), None),
        ),
        out_specs=(P("strike", "depth"), P("strike", "depth"), P(None, ("strike", "depth"), None)),
        check_vma=False,
    )
```
